128 devices in a mesh: problem: 1, samp: 2 (over core), feat: 64 (over z, y, x).
Axes of the slice: x: 4, y: 4, z: 4, core: 2. Of those that a mesh axis runs over, the one named last changes fastest.
Arguments:
- design: bfloat16 [4096, 131072], P(('problem', 'samp'), 'feat')
- targets: float32 [4096, 128], P(('problem', 'samp'))
- coef_init: float32 [131072, 128], P(('problem', 'feat'))
- step_sizes: float32 [131072], P(('problem', 'feat'))
- ridge_weights: float32 [128], P('problem')
Outputs:
- output 1: float32 [131072, 128], P(('problem', 'feat'))
- output 2: float32 [4096, 128], P(('problem', 'samp'))
All inputs are finite; a program needn't handle non-finite values.
Results may differ from the reference program's by a relative error of at most 0.00658185.
Values are sent between devices in bfloat16 or wider.
A program may use at most 1 GiB of HBM per device.

```python
import jax
import jax.numpy as jnp
from jax import lax

NUM_ROWS = 4096
NUM_FEATURES = 131072
NUM_TARGETS = 128
FEAT_BLOCKS = 64
SWEEPS = 4
STEP_WEIGHT = 0.5


def setup_inputs(seed: int = 0, part: int = 0) -> dict:
    base_key = jax.random.fold_in(jax.random.key(seed), part)
    sub_keys = jax.random.split(base_key, 9)
    shared_rank = 8
    shared_mix = 0.8
    row_block = NUM_ROWS // 8
    factors = jax.random.normal(sub_keys[0], (NUM_ROWS, shared_rank), jnp.float32)
    loadings = jax.random.normal(sub_keys[1], (shared_rank, NUM_FEATURES), jnp.float32)

    def draw_rows(block_index):
        rows_f = lax.dynamic_slice_in_dim(factors, block_index * row_block, row_block, 0)
        shared = jnp.dot(rows_f, loadings) * (shared_mix / shared_rank) ** 0.5
        noise_blk = jax.random.normal(jax.random.fold_in(sub_keys[2], block_index), (row_block, NUM_FEATURES), jnp.float32)
        return (shared + (1.0 - shared_mix) ** 0.5 * noise_blk).astype(jnp.bfloat16)

    design = lax.map(draw_rows, jnp.arange(8)).reshape(NUM_ROWS, NUM_FEATURES)

    def power_step(step_index, probe_vec):
        unit_vec = probe_vec / jnp.linalg.norm(probe_vec)
        image_vec = jnp.dot(design, unit_vec.astype(jnp.bfloat16), preferred_element_type=jnp.float32)
        return jnp.dot(image_vec.astype(jnp.bfloat16), design, preferred_element_type=jnp.float32) / NUM_ROWS

    probe_init = jax.random.normal(sub_keys[3], (NUM_FEATURES,), jnp.float32)
    curvature = 1.15 * jnp.linalg.norm(lax.fori_loop(0, 12, power_step, probe_init))
    step_sizes = jax.random.uniform(sub_keys[4], (NUM_FEATURES,), jnp.float32, 0.4, 0.8) / curvature
    ridge_weights = jax.random.uniform(sub_keys[5], (NUM_TARGETS,), jnp.float32, 0.05, 0.25) * curvature
    coef_init = jax.random.normal(sub_keys[6], (NUM_FEATURES, NUM_TARGETS), jnp.float32) * NUM_FEATURES ** -0.5
    w_star = jax.random.normal(sub_keys[7], (NUM_FEATURES, NUM_TARGETS), jnp.float32) * NUM_FEATURES ** -0.5
    targets = jnp.dot(design, w_star.astype(jnp.bfloat16), preferred_element_type=jnp.float32) + 0.3 * jax.random.normal(sub_keys[8], (NUM_ROWS, NUM_TARGETS), jnp.float32)
    return {"design": design, "targets": targets, "coef_init": coef_init, "step_sizes": step_sizes, "ridge_weights": ridge_weights}


def reference(design, targets, coef_init, step_sizes, ridge_weights):
    block_cols = NUM_FEATURES // FEAT_BLOCKS

    def block_sum(weights):
        weights_b = weights.astype(jnp.bfloat16)

        def add_block(acc_sum, block_index):
            col_block = lax.dynamic_slice_in_dim(design, block_index * block_cols, block_cols, 1)
            rows_w = lax.dynamic_slice_in_dim(weights_b, block_index * block_cols, block_cols, 0)
            product = jnp.dot(col_block, rows_w, preferred_element_type=jnp.float32)
            return acc_sum + product.astype(jnp.bfloat16).astype(jnp.float32), None

        return lax.scan(add_block, jnp.zeros((NUM_ROWS, NUM_TARGETS), jnp.float32), jnp.arange(FEAT_BLOCKS))[0]

    def sweep_once(sweep_state, unused):
        coef_cur, resid_cur = sweep_state
        gradient = lax.dot_general(design, resid_cur.astype(jnp.bfloat16), (((0,), (0,)), ((), ())), preferred_element_type=jnp.float32) / NUM_ROWS
        step_delta = step_sizes[:, None] * (gradient - ridge_weights[None, :] * coef_cur)
        return (coef_cur + STEP_WEIGHT * step_delta, resid_cur - STEP_WEIGHT * block_sum(step_delta)), None

    start_state = (coef_init, targets - block_sum(coef_init))
    final_state = lax.scan(sweep_once, start_state, None, length=SWEEPS)[0]
    return final_state[0], final_state[1]
```

```python
import functools

import jax
import jax.numpy as jnp
from jax import lax
from jax.experimental import pallas as pl
from jax.experimental.pallas import tpu as pltpu
from jax.sharding import PartitionSpec as P

SWEEPS = 4
STEP_WEIGHT = 0.5
FT = 256


def _kernel(side, n_feat, n_samp, x_hbm, y_hbm, w0_hbm, eta_ref, lam_ref, w_out, r_out,
            x_v, w_nat, w_t, sb, u_buf, rs_recv, rb_full, gt, g_recv, rs_res, rf_full, rf_own,
            x_sem, in_sem, rs_ssem, rs_rsem, ag_ssem, ag_rsem, g_ssem, g_rsem, out_sem):
    rows, feats = x_v.shape
    targets = w_nat.shape[1]
    own = rows // n_feat
    per_z = n_feat // side
    zrows = rows // side
    n_ft = feats // FT
    total_rows = rows * n_samp

    me = lax.axis_index("feat")
    core = lax.axis_index("samp")
    mz, my, mx = me // (side * side), (me // side) % side, me % side

    def peer_of(dz, dy, dx):
        return ((mz + dz) % side) * (side * side) + ((my + dy) % side) * side + (mx + dx) % side

    barrier = pltpu.get_barrier_semaphore()
    for d in range(1, n_feat):
        pl.semaphore_signal(barrier, inc=1, device_id={"feat": peer_of(d // (side * side), (d // side) % side, d % side)},
                            device_id_type=pl.DeviceIdType.MESH)
    pl.semaphore_signal(barrier, inc=1, device_id={"samp": 1 - core}, device_id_type=pl.DeviceIdType.MESH)

    w_load = pltpu.make_async_copy(w0_hbm, w_nat, in_sem.at[0])
    w_load.start()

    def x_load(k):
        z_rows = pl.ds(pl.multiple_of(((mz + k + 1) % side) * zrows, zrows), zrows)
        return pltpu.make_async_copy(x_hbm.at[z_rows], x_v.at[z_rows], x_sem.at[k])

    for k in range(side):
        x_load(k).start()
    y_load = pltpu.make_async_copy(y_hbm.at[pl.ds(pl.multiple_of(me * own, own), own)], rs_res, in_sem.at[1])
    y_load.start()

    def rs_copy(slot, peer):
        return pltpu.make_async_remote_copy(src_ref=u_buf.at[peer], dst_ref=rs_recv.at[slot], send_sem=rs_ssem, recv_sem=rs_rsem,
                                            device_id={"feat": peer}, device_id_type=pl.DeviceIdType.MESH)

    def rs_all():
        return pltpu.make_async_remote_copy(src_ref=u_buf.at[pl.ds(1, n_feat - 1)], dst_ref=rs_recv.at[pl.ds(1, n_feat - 1)],
                                            send_sem=rs_ssem, recv_sem=rs_rsem, device_id={"feat": me},
                                            device_id_type=pl.DeviceIdType.MESH)

    def product_and_send(k):
        pz = (mz + k + 1) % side
        z_rows = pl.ds(pl.multiple_of(pz * zrows, zrows), zrows)
        u = jnp.dot(x_v[z_rows, :], sb[...], preferred_element_type=jnp.float32)
        u_buf[pl.ds(pz * per_z, per_z)] = u.astype(jnp.bfloat16).reshape(per_z, own, targets)
        dz = (k + 1) % side
        for dy in range(side - 1, -1, -1):
            for dx in range(side - 1, -1, -1):
                peer = peer_of(dz, dy, dx)
                slot = dz * side * side + dy * side + dx
                if dy == 0 and dx == 0:
                    @pl.when(dz != 0)
                    def _():
                        rs_copy(slot, peer).start()
                else:
                    rs_copy(slot, peer).start()

    def reduced():
        rs_all().wait_recv()
        acc = u_buf[me].astype(jnp.float32)
        for d in range(1, n_feat):
            acc = acc + rs_recv[d].astype(jnp.float32)
        return acc

    def gather_copies(src_ref, dst_ref):
        out = []
        for d in range(n_feat - 1, 0, -1):
            peer = peer_of(d // (side * side), (d // side) % side, d % side)
            out.append(pltpu.make_async_remote_copy(src_ref=src_ref, dst_ref=dst_ref.at[me], send_sem=ag_ssem, recv_sem=ag_rsem,
                                                    device_id={"feat": peer}, device_id_type=pl.DeviceIdType.MESH))
        return out

    def gather_all(ref):
        part = ref.at[pl.ds(1, n_feat - 1)]
        return pltpu.make_async_remote_copy(src_ref=part, dst_ref=part, send_sem=ag_ssem, recv_sem=ag_rsem, device_id={"feat": me},
                                            device_id_type=pl.DeviceIdType.MESH)

    def g_copy(par, f):
        return pltpu.make_async_remote_copy(src_ref=gt.at[f], dst_ref=g_recv.at[par, f], send_sem=g_ssem.at[f],
                                            recv_sem=g_rsem.at[par, f], device_id={"samp": 1 - core},
                                            device_id_type=pl.DeviceIdType.MESH)

    w_load.wait()
    sb[...] = w_nat[...].astype(jnp.bfloat16)
    x_load(0).wait()
    pl.semaphore_wait(barrier, n_feat)

    def first(k, _):
        @pl.when(k > 0)
        def _():
            x_load(k).wait()
        product_and_send(k)
        return 0

    lax.fori_loop(0, side, first, 0)
    for f in range(n_ft):
        w_t[f] = w_nat[f * FT:(f + 1) * FT, :].T
    lam_t = jnp.broadcast_to(lam_ref[...], (targets, targets)).T
    lam_tile = jnp.concatenate([lam_t] * (FT // targets), axis=1)
    y_load.wait()
    rs_res[...] = rs_res[...] - reduced()
    rs_all().wait_send()

    def sweep(s, _):
        par = s % 2
        rb_full[me] = rs_res[...].astype(jnp.bfloat16)
        for c in gather_copies(rb_full.at[me], rb_full):
            c.start()
        gather_all(rb_full).wait_recv()
        rbt = rb_full[...].reshape(rows, targets).T

        def grad(f, _):
            cols = pl.ds(pl.multiple_of(f * FT, FT), FT)
            gt[f] = jnp.dot(rbt, x_v[:, cols], preferred_element_type=jnp.float32)
            g_copy(par, f).start()
            return 0

        lax.fori_loop(0, n_ft, grad, 0)
        gather_all(rb_full).wait_send()

        def step(f, _):
            g_copy(par, f).wait_recv()
            cols = pl.ds(pl.multiple_of(f * FT, FT), FT)
            gradient = (gt[f] + g_recv[par, f]) / total_rows
            w = w_t[f]
            delta = eta_ref[:, cols] * (gradient - lam_tile * w)
            w_t[f] = w + STEP_WEIGHT * delta
            sb[cols, :] = delta.astype(jnp.bfloat16).T
            return 0

        lax.fori_loop(0, n_ft, step, 0)
        lax.fori_loop(0, side, lambda k, _: (product_and_send(k), 0)[1], 0)
        for f in range(n_ft):
            g_copy(par, f).wait_send()

        @pl.when(s == SWEEPS - 1)
        def _():
            for f in range(n_ft):
                w_nat[f * FT:(f + 1) * FT, :] = w_t[f].T
            pltpu.make_async_copy(w_nat, w_out, out_sem.at[0]).start()

        rs_res[...] = rs_res[...] - STEP_WEIGHT * reduced()
        rs_all().wait_send()
        return 0

    lax.fori_loop(0, SWEEPS, sweep, 0)

    rf_full[me] = rs_res[...]
    for c in gather_copies(rf_full.at[me], rf_full):
        c.start()
    gather_all(rf_full).wait_recv()
    r_copy = pltpu.make_async_copy(rf_full, r_out, out_sem.at[1])
    r_copy.start()
    gather_all(rf_full).wait_send()
    pltpu.make_async_copy(w_nat, w_out, out_sem.at[0]).wait()
    r_copy.wait()


def solution(mesh):
    n_samp, n_feat = mesh.shape["samp"], mesh.shape["feat"]
    side = round(n_feat ** (1 / 3))
    design_spec = P(("problem", "samp"), "feat")
    rows_spec = P(("problem", "samp"), None)
    coef_spec = P(("problem", "feat"), None)
    step_spec = P(("problem", "feat"))
    ridge_spec = P("problem")

    def local_sweeps(design, targets, coef_init, step_sizes, ridge_weights):
        rows, feats = design.shape
        tgt = targets.shape[1]
        own = rows // n_feat
        n_ft = feats // FT
        f32, bf16 = jnp.float32, jnp.bfloat16
        hbm = pl.BlockSpec(memory_space=pl.ANY)
        vmem = pl.BlockSpec(memory_space=pltpu.VMEM)
        w, r = pl.pallas_call(
            functools.partial(_kernel, side, n_feat, n_samp),
            name="descent",
            out_shape=(jax.ShapeDtypeStruct((feats, tgt), f32), jax.ShapeDtypeStruct((n_feat, own, tgt), f32)),
            in_specs=[hbm, hbm, hbm, vmem, vmem],
            out_specs=(hbm, hbm),
            scratch_shapes=[
                pltpu.VMEM((rows, feats), bf16),
                pltpu.VMEM((feats, tgt), f32),
                pltpu.VMEM((n_ft, tgt, FT), f32),
                pltpu.VMEM((feats, tgt), bf16),
                pltpu.VMEM((n_feat, own, tgt), bf16),
                pltpu.VMEM((n_feat, own, tgt), bf16),
                pltpu.VMEM((n_feat, own, tgt), bf16),
                pltpu.VMEM((n_ft, tgt, FT), f32),
                pltpu.VMEM((2, n_ft, tgt, FT), f32),
                pltpu.VMEM((own, tgt), f32),
                pltpu.VMEM((n_feat, own, tgt), f32),
                pltpu.VMEM((own, tgt), f32),
                pltpu.SemaphoreType.DMA((side,)),
                pltpu.SemaphoreType.DMA((2,)),
                pltpu.SemaphoreType.DMA,
                pltpu.SemaphoreType.DMA,
                pltpu.SemaphoreType.DMA,
                pltpu.SemaphoreType.DMA,
                pltpu.SemaphoreType.DMA((n_ft,)),
                pltpu.SemaphoreType.DMA((2, n_ft)),
                pltpu.SemaphoreType.DMA((2,)),
            ],
            compiler_params=pltpu.CompilerParams(collective_id=0, has_side_effects=True, vmem_limit_bytes=56 * 1024 * 1024),
        )(design, targets, coef_init, step_sizes[None, :], ridge_weights[None, :])
        return w, r.reshape(rows, tgt)

    return jax.shard_map(local_sweeps, mesh=mesh, in_specs=(design_spec, rows_spec, coef_spec, step_spec, ridge_spec), out_specs=(coef_spec, rows_spec), check_vma=False)
```

```python
import functools

import jax
import jax.numpy as jnp
from jax import lax
from jax.experimental import pallas as pl
from jax.experimental.pallas import tpu as pltpu
from jax.sharding import PartitionSpec as P

SWEEPS = 4
STEP_WEIGHT = 0.5
CHAINS = 2
TILE = 128
BIG = 512
MESH = pl.DeviceIdType.MESH


def _kernel(n_feat, n_samp, x_hbm, y_hbm, w0_hbm, eta_ref, lam_ref, w_out, r_out,
            x_v, w_nat, w_t, st, u_buf, rs_recv, rb_full, gt, g_recv, rs_res, rf_full, y_tile, lam_t,
            x_sem, in_sem, rs_ssem, rs_rsem, ag_ssem, ag_rsem, g_ssem, g_rsem, out_sem):
    rows, feats = x_v.shape
    targets = w_nat.shape[1]
    half = targets // CHAINS
    n_sg = rows // TILE
    n_tg = n_feat // n_sg
    th = half // n_tg
    n_fb, n_sb = feats // BIG, rows // BIG
    per_sb = n_feat // n_sb
    total_rows = rows * n_samp

    me = lax.axis_index("feat")
    core = lax.axis_index("samp")

    barrier = pltpu.get_barrier_semaphore()

    def greet(d, _):
        pl.semaphore_signal(barrier, inc=1, device_id={"feat": (me + d) % n_feat}, device_id_type=MESH)
        return 0

    lax.fori_loop(1, n_feat, greet, 0)
    pl.semaphore_signal(barrier, inc=1, device_id={"samp": 1 - core}, device_id_type=MESH)

    w_load = pltpu.make_async_copy(w0_hbm, w_nat, in_sem.at[0])
    w_load.start()

    my_sb = me // per_sb

    def block_rows(k):
        return pl.ds(pl.multiple_of(((my_sb + k + 1) % n_sb) * BIG, BIG), BIG)

    def x_load(k):
        return pltpu.make_async_copy(x_hbm.at[block_rows(k)], x_v.at[block_rows(k)], x_sem.at[k])

    for k in range(n_sb):
        x_load(k).start()
    my_sg, my_tg = me // n_tg, me % n_tg
    y_load = pltpu.make_async_copy(y_hbm.at[pl.ds(pl.multiple_of(my_sg * TILE, TILE), TILE)], y_tile, in_sem.at[1])
    y_load.start()

    def rs_copy(c, peer):
        return pltpu.make_async_remote_copy(src_ref=u_buf.at[c, peer], dst_ref=rs_recv.at[c, me], send_sem=rs_ssem.at[c],
                                            recv_sem=rs_rsem.at[c], device_id={"feat": peer}, device_id_type=MESH)

    def rs_all(c):
        return pltpu.make_async_remote_copy(src_ref=u_buf.at[c, pl.ds(1, n_feat - 1)], dst_ref=rs_recv.at[c, pl.ds(1, n_feat - 1)],
                                            send_sem=rs_ssem.at[c], recv_sem=rs_rsem.at[c], device_id={"feat": me},
                                            device_id_type=MESH)

    def product_and_send(c, k):
        sb = (my_sb + k + 1) % n_sb
        u = lax.dot_general(st[c], x_v[block_rows(k), :], (((1,), (1,)), ((), ())), preferred_element_type=jnp.float32)
        for j in range(per_sb):
            g, t = j // n_tg, j % n_tg
            part = u[t * th:(t + 1) * th, g * TILE:(g + 1) * TILE].astype(jnp.bfloat16)
            u_buf[c, sb * per_sb + j] = part
        for i in range(per_sb):
            peer = sb * per_sb + (my_in_sb + i) % per_sb
            if i == 0:
                @pl.when(k != n_sb - 1)
                def _():
                    rs_copy(c, peer).start()
            else:
                rs_copy(c, peer).start()

    my_in_sb = me % per_sb

    def reduce(c, coef):
        rs_all(c).wait_recv()
        rs_recv[c, me] = u_buf[c, me]
        accs = [rs_recv[c, j].astype(jnp.float32) for j in range(4)]
        for j in range(4, n_feat):
            accs[j % 4] = accs[j % 4] + rs_recv[c, j].astype(jnp.float32)
        total = (accs[0] + accs[1]) + (accs[2] + accs[3])
        rs_res[c] = rs_res[c] - coef * total

    def gather_start(c, ref):
        def send(d, _):
            peer = (me + n_feat // 2 + d) % n_feat
            @pl.when(peer != me)
            def _():
                pltpu.make_async_remote_copy(src_ref=ref.at[c, me], dst_ref=ref.at[c, me], send_sem=ag_ssem.at[c],
                                             recv_sem=ag_rsem.at[c], device_id={"feat": peer}, device_id_type=MESH).start()
            return 0
        lax.fori_loop(0, n_feat, send, 0, unroll=8)

    def gather_all(c, ref):
        part = ref.at[c, pl.ds(1, n_feat - 1)]
        return pltpu.make_async_remote_copy(src_ref=part, dst_ref=part, send_sem=ag_ssem.at[c], recv_sem=ag_rsem.at[c],
                                            device_id={"feat": me}, device_id_type=MESH)

    def g_copy(c, par, f):
        return pltpu.make_async_remote_copy(src_ref=gt.at[c, f], dst_ref=g_recv.at[par, c, f], send_sem=g_ssem.at[c, f],
                                            recv_sem=g_rsem.at[par, c, f], device_id={"samp": 1 - core}, device_id_type=MESH)

    w_load.wait()
    for f in range(n_fb):
        wt = w_nat[f * BIG:(f + 1) * BIG, :].T
        for c in range(CHAINS):
            w_t[c, f] = wt[c * half:(c + 1) * half]
            st[c, :, f * BIG:(f + 1) * BIG] = wt[c * half:(c + 1) * half].astype(jnp.bfloat16)
    lam_t[...] = jnp.broadcast_to(lam_ref[...], (targets, targets)).T
    x_load(0).wait()
    pl.semaphore_wait(barrier, n_feat)

    def first(i, _):
        c, k = i // n_sb, i % n_sb
        @pl.when((i > 0) & (i < n_sb))
        def _():
            x_load(k).wait()
        product_and_send(c, k)
        return 0

    lax.fori_loop(0, CHAINS * n_sb, first, 0)
    y_load.wait()
    y_tile[...] = y_tile[...].T

    def first_reduce(c, _):
        rs_res[c] = y_tile[pl.ds(pl.multiple_of(c * half + my_tg * th, th), th), :]
        reduce(c, 1.0)
        rb_full[c, me] = rs_res[c].astype(jnp.bfloat16)
        gather_start(c, rb_full)
        rs_all(c).wait_send()
        return 0

    lax.fori_loop(0, CHAINS, first_reduce, 0)

    def sweep(s, _):
        par = s % 2

        def ahead(c, _):
            gather_all(c, rb_full).wait_recv()
            rbt = jnp.concatenate([rb_full[c, g * n_tg:(g + 1) * n_tg].reshape(half, TILE) for g in range(n_sg)], axis=1)

            def grad(f, _):
                cols = pl.ds(pl.multiple_of(f * BIG, BIG), BIG)
                gt[c, f] = jnp.dot(rbt, x_v[:, cols], preferred_element_type=jnp.float32)
                g_copy(c, par, f).start()
                return 0

            lax.fori_loop(0, n_fb, grad, 0)
            gather_all(c, rb_full).wait_send()
            lam = lam_t[pl.ds(pl.multiple_of(c * half, half), half), :]
            lam = jnp.concatenate([lam] * (BIG // targets), axis=1)

            def step(f, _):
                g_copy(c, par, f).wait_recv()
                cols = pl.ds(pl.multiple_of(f * BIG, BIG), BIG)
                gradient = (gt[c, f] + g_recv[par, c, f]) / total_rows
                w = w_t[c, f]
                delta = eta_ref[:, cols] * (gradient - lam * w)
                w_t[c, f] = w + STEP_WEIGHT * delta
                st[c, :, cols] = delta.astype(jnp.bfloat16)
                return 0

            lax.fori_loop(0, n_fb, step, 0)
            lax.fori_loop(0, n_sb, lambda k, _: (product_and_send(c, k), 0)[1], 0)
            for f in range(n_fb):
                g_copy(c, par, f).wait_send()
            return 0

        lax.fori_loop(0, CHAINS, ahead, 0)

        @pl.when(s == SWEEPS - 1)
        def _():
            for f in range(n_fb):
                w_nat[f * BIG:(f + 1) * BIG, :] = jnp.concatenate([w_t[c, f] for c in range(CHAINS)], axis=0).T
            pltpu.make_async_copy(w_nat, w_out, out_sem.at[0]).start()

        def behind(c, _):
            reduce(c, STEP_WEIGHT)

            @pl.when(s < SWEEPS - 1)
            def _():
                rb_full[c, me] = rs_res[c].astype(jnp.bfloat16)
                gather_start(c, rb_full)

            @pl.when(s == SWEEPS - 1)
            def _():
                rf_full[c, me] = rs_res[c]
                gather_start(c, rf_full)

            rs_all(c).wait_send()
            return 0

        lax.fori_loop(0, CHAINS, behind, 0)
        return 0

    lax.fori_loop(0, SWEEPS, sweep, 0)

    for c in range(CHAINS):
        gather_all(c, rf_full).wait_recv()
    pltpu.make_async_copy(w_nat, w_out, out_sem.at[0]).wait()
    for g in range(n_sg):
        both = jnp.concatenate([rf_full[c, g * n_tg:(g + 1) * n_tg].reshape(half, TILE) for c in range(CHAINS)], axis=0)
        w_nat[g * TILE:(g + 1) * TILE, :] = both.T
    r_copy = pltpu.make_async_copy(w_nat, r_out, out_sem.at[1])
    r_copy.start()
    for c in range(CHAINS):
        gather_all(c, rf_full).wait_send()
    r_copy.wait()


def solution(mesh):
    n_samp, n_feat = mesh.shape["samp"], mesh.shape["feat"]
    design_spec = P(("problem", "samp"), "feat")
    rows_spec = P(("problem", "samp"), None)
    coef_spec = P(("problem", "feat"), None)
    step_spec = P(("problem", "feat"))
    ridge_spec = P("problem")

    def local_sweeps(design, targets, coef_init, step_sizes, ridge_weights):
        rows, feats = design.shape
        tgt = targets.shape[1]
        half = tgt // CHAINS
        n_fb, n_sb = feats // BIG, rows // BIG
        n_tg = n_feat // (rows // TILE)
        th = half // n_tg
        f32, bf16 = jnp.float32, jnp.bfloat16
        hbm = pl.BlockSpec(memory_space=pl.ANY)
        vmem = pl.BlockSpec(memory_space=pltpu.VMEM)
        return pl.pallas_call(
            functools.partial(_kernel, n_feat, n_samp),
            name="descent",
            out_shape=(jax.ShapeDtypeStruct((feats, tgt), f32), jax.ShapeDtypeStruct((rows, tgt), f32)),
            in_specs=[hbm, hbm, hbm, vmem, vmem],
            out_specs=(hbm, hbm),
            scratch_shapes=[
                pltpu.VMEM((rows, feats), bf16),
                pltpu.VMEM((feats, tgt), f32),
                pltpu.VMEM((CHAINS, n_fb, half, BIG), f32),
                pltpu.VMEM((CHAINS, half, feats), bf16),
                pltpu.VMEM((CHAINS, n_feat, th, TILE), bf16),
                pltpu.VMEM((CHAINS, n_feat, th, TILE), bf16),
                pltpu.VMEM((CHAINS, n_feat, th, TILE), bf16),
                pltpu.VMEM((CHAINS, n_fb, half, BIG), f32),
                pltpu.VMEM((2, CHAINS, n_fb, half, BIG), f32),
                pltpu.VMEM((CHAINS, th, TILE), f32),
                pltpu.VMEM((CHAINS, n_feat, th, TILE), f32),
                pltpu.VMEM((TILE, tgt), f32),
                pltpu.VMEM((tgt, tgt), f32),
                pltpu.SemaphoreType.DMA((n_sb,)),
                pltpu.SemaphoreType.DMA((2,)),
                pltpu.SemaphoreType.DMA((CHAINS,)),
                pltpu.SemaphoreType.DMA((CHAINS,)),
                pltpu.SemaphoreType.DMA((CHAINS,)),
                pltpu.SemaphoreType.DMA((CHAINS,)),
                pltpu.SemaphoreType.DMA((CHAINS, n_fb)),
                pltpu.SemaphoreType.DMA((2, CHAINS, n_fb)),
                pltpu.SemaphoreType.DMA((2,)),
            ],
            compiler_params=pltpu.CompilerParams(collective_id=0, has_side_effects=True, vmem_limit_bytes=56 * 1024 * 1024),
        )(design, targets, coef_init, step_sizes[None, :], ridge_weights[None, :])

    return jax.shard_map(local_sweeps, mesh=mesh, in_specs=(design_spec, rows_spec, coef_spec, step_spec, ridge_spec), out_specs=(coef_spec, rows_spec), check_vma=False)
```

```python
import functools

import jax
import jax.numpy as jnp
from jax import lax
from jax.experimental import pallas as pl
from jax.experimental.pallas import tpu as pltpu
from jax.sharding import PartitionSpec as P

SWEEPS = 4
STEP_WEIGHT = 0.5
CHAINS = 2
TILE = 128
BIG = 512
MESH = pl.DeviceIdType.MESH


def _kernel(side, n_feat, n_samp, x_hbm, y_hbm, w0_hbm, eta_ref, lam_ref, w_out, r_out,
            x_v, xt_v, w_nat, w_t, st, u_buf, rs_recv, rb_full, gt, g_recv, rs_res, rf_full, y_tile, lam_t,
            x_sem, in_sem, rs_ssem, rs_rsem, ag_ssem, ag_psem, ag_rsem, g_ssem, g_rsem, out_sem):
    rows, feats = x_v.shape
    targets = w_nat.shape[1]
    half = targets // CHAINS
    n_sg = rows // TILE
    n_tg = n_feat // n_sg
    th = half // n_tg
    n_fb, n_sb = feats // BIG, rows // BIG
    per_sb = n_feat // n_sb
    total_rows = rows * n_samp

    me = lax.axis_index("feat")
    core = lax.axis_index("samp")

    barrier = pltpu.get_barrier_semaphore()

    def greet(d, _):
        pl.semaphore_signal(barrier, inc=1, device_id={"feat": (me + d) % n_feat}, device_id_type=MESH)
        return 0

    lax.fori_loop(1, n_feat, greet, 0)
    pl.semaphore_signal(barrier, inc=1, device_id={"samp": 1 - core}, device_id_type=MESH)

    w_load = pltpu.make_async_copy(w0_hbm, w_nat, in_sem.at[0])
    w_load.start()

    my_sb = me // per_sb

    def block_rows(k):
        return pl.ds(pl.multiple_of(((my_sb + k + 1) % n_sb) * BIG, BIG), BIG)

    def x_load(k):
        return pltpu.make_async_copy(x_hbm.at[block_rows(k)], x_v.at[block_rows(k)], x_sem.at[k])

    for k in range(n_sb):
        x_load(k).start()
    my_sg, my_tg = me // n_tg, me % n_tg
    y_load = pltpu.make_async_copy(y_hbm.at[pl.ds(pl.multiple_of(my_sg * TILE, TILE), TILE)], y_tile, in_sem.at[1])
    y_load.start()

    def rs_copy(c, peer):
        return pltpu.make_async_remote_copy(src_ref=u_buf.at[c, peer], dst_ref=rs_recv.at[c, me], send_sem=rs_ssem.at[c],
                                            recv_sem=rs_rsem.at[c], device_id={"feat": peer}, device_id_type=MESH)

    def rs_all(c):
        return pltpu.make_async_remote_copy(src_ref=u_buf.at[c, pl.ds(1, n_feat - 1)], dst_ref=rs_recv.at[c, pl.ds(1, n_feat - 1)],
                                            send_sem=rs_ssem.at[c], recv_sem=rs_rsem.at[c], device_id={"feat": me},
                                            device_id_type=MESH)

    my_in_sb = me % per_sb

    def send_tiles(c, k, u):
        sb = (my_sb + k + 1) % n_sb
        for j in range(per_sb):
            g, t = j // n_tg, j % n_tg
            u_buf[c, sb * per_sb + j] = u[t * th:(t + 1) * th, g * TILE:(g + 1) * TILE].astype(jnp.bfloat16)
        for i in range(per_sb):
            peer = sb * per_sb + (my_in_sb + i) % per_sb
            if i == 0:
                @pl.when(k != n_sb - 1)
                def _():
                    rs_copy(c, peer).start()
            else:
                rs_copy(c, peer).start()

    def reduce(c, coef):
        rs_all(c).wait_recv()
        rs_recv[c, me] = u_buf[c, me]
        accs = [rs_recv[c, j].astype(jnp.float32) for j in range(4)]
        for j in range(4, n_feat):
            accs[j % 4] = accs[j % 4] + rs_recv[c, j].astype(jnp.float32)
        total = (accs[0] + accs[1]) + (accs[2] + accs[3])
        rs_res[c] = rs_res[c] - coef * total

    def axes(c):
        third = (c * n_samp + core) % 3
        strides = [jnp.where(d == 0, 1, jnp.where(d == 1, side, side * side)) for d in (third, (third + 1) % 3, (third + 2) % 3)]
        return [(stride, (me // stride) % side) for stride in strides]

    def moved(axis, by):
        stride, at = axis
        return ((at + by) % side - at) * stride

    def hops(d):
        return min(d, side - d)

    plane = sorted([(a, b) for a in range(side) for b in range(side) if a or b], key=lambda o: hops(o[0]) + hops(o[1]))

    def pass_on(c, ref, owner):
        ring = axes(c)[0]
        for d in range(side - 1, 0, -1):
            pltpu.make_async_remote_copy(src_ref=ref.at[c, owner], dst_ref=ref.at[c, owner], send_sem=ag_ssem.at[c],
                                         recv_sem=ag_rsem.at[c], device_id={"feat": me + moved(ring, d)}, device_id_type=MESH).start()

    def plane_copy(c, ref, i, owner, peer):
        return pltpu.make_async_remote_copy(src_ref=ref.at[c, owner], dst_ref=ref.at[c, owner], send_sem=ag_ssem.at[c],
                                            recv_sem=ag_psem.at[c, i], device_id={"feat": peer}, device_id_type=MESH)

    def gather_start(c, ref):
        _, one, two = axes(c)
        for i in range(len(plane) - 1, -1, -1):
            a, b = plane[i]
            plane_copy(c, ref, i, me, me + moved(one, a) + moved(two, b)).start()
        pass_on(c, ref, me)

    def gather_forward(c, ref):
        _, one, two = axes(c)
        for i, (a, b) in enumerate(plane):
            owner = me + moved(one, side - a) + moved(two, side - b)
            plane_copy(c, ref, i, owner, me).wait_recv()
            pass_on(c, ref, owner)

    def gather_wait(c, ref):
        part = ref.at[c, pl.ds(0, n_feat - side * side)]
        pltpu.make_async_remote_copy(src_ref=part, dst_ref=part, send_sem=ag_ssem.at[c], recv_sem=ag_rsem.at[c],
                                     device_id={"feat": me}, device_id_type=MESH).wait_recv()

    def gather_sent(c, ref):
        part = ref.at[c, pl.ds(1, n_feat - 1)]
        pltpu.make_async_remote_copy(src_ref=part, dst_ref=part, send_sem=ag_ssem.at[c], recv_sem=ag_rsem.at[c],
                                     device_id={"feat": me}, device_id_type=MESH).wait_send()

    def g_copy(c, par, f):
        return pltpu.make_async_remote_copy(src_ref=gt.at[c, f], dst_ref=g_recv.at[par, c, f], send_sem=g_ssem.at[c, f],
                                            recv_sem=g_rsem.at[par, c, f], device_id={"samp": 1 - core}, device_id_type=MESH)

    w_load.wait()
    for f in range(n_fb):
        wt = w_nat[f * BIG:(f + 1) * BIG, :].T
        for c in range(CHAINS):
            w_t[c, f] = wt[c * half:(c + 1) * half]
            st[c, :, f * BIG:(f + 1) * BIG] = wt[c * half:(c + 1) * half].astype(jnp.bfloat16)
    lam_t[...] = jnp.broadcast_to(lam_ref[...], (targets, targets)).T
    x_load(0).wait()
    pl.semaphore_wait(barrier, n_feat)

    def first(k, _):
        @pl.when(k > 0)
        def _():
            x_load(k).wait()
        u = lax.dot_general(st[...].reshape(targets, feats), x_v[block_rows(k), :], (((1,), (1,)), ((), ())),
                            preferred_element_type=jnp.float32)
        for c in range(CHAINS):
            send_tiles(c, k, u[c * half:(c + 1) * half])
        return 0

    lax.fori_loop(0, n_sb, first, 0)

    def turn(r, _):
        piece = pl.ds(pl.multiple_of(r * TILE, TILE), TILE)
        xt_v[:, piece] = x_v[piece, :].T
        return 0

    lax.fori_loop(0, n_sg, turn, 0)
    y_load.wait()
    y_tile[...] = y_tile[...].T

    def behind(c, coef, last):
        reduce(c, coef)
        if last:
            rf_full[c, me] = rs_res[c]
        else:
            rb_full[c, me] = rs_res[c].astype(jnp.bfloat16)
        gather_start(c, rf_full if last else rb_full)
        rs_all(c).wait_send()

    def gradient_part(c, par):
        gather_wait(c, rb_full)
        rbt = jnp.concatenate([rb_full[c, g * n_tg:(g + 1) * n_tg].reshape(half, TILE) for g in range(n_sg)], axis=1)

        def grad(f, _):
            cols = pl.ds(pl.multiple_of(f * BIG, BIG), BIG)
            gt[c, f] = jnp.dot(rbt, x_v[:, cols], preferred_element_type=jnp.float32)
            g_copy(c, par, f).start()
            return 0

        lax.fori_loop(0, n_fb, grad, 0)

    def step_and_product(c, par):
        lam = lam_t[c * half:(c + 1) * half, :]
        lam = jnp.concatenate([lam] * (BIG // targets), axis=1)

        def step(f, _):
            g_copy(c, par, f).wait_recv()
            cols = pl.ds(pl.multiple_of(f * BIG, BIG), BIG)
            gradient = (gt[c, f] + g_recv[par, c, f]) / total_rows
            w = w_t[c, f]
            delta = eta_ref[:, cols] * (gradient - lam * w)
            w_t[c, f] = w + STEP_WEIGHT * delta
            st[c, :, cols] = delta.astype(jnp.bfloat16)
            return 0

        lax.fori_loop(0, n_fb, step, 0)
        gather_sent(c, rb_full)

        def product(k, _):
            send_tiles(c, k, jnp.dot(st[c], xt_v[:, block_rows(k)], preferred_element_type=jnp.float32))
            return 0

        lax.fori_loop(0, n_sb, product, 0)
        for f in range(n_fb):
            g_copy(c, par, f).wait_send()

    def sweep(s, last):
        par = s % 2
        gradient_part(0, par)
        gather_forward(1, rb_full)
        step_and_product(0, par)
        gradient_part(1, par)
        step_and_product(1, par)
        if last:
            for f in range(n_fb):
                w_nat[f * BIG:(f + 1) * BIG, :] = jnp.concatenate([w_t[c, f] for c in range(CHAINS)], axis=0).T
            pltpu.make_async_copy(w_nat, w_out, out_sem.at[0]).start()
        behind(0, STEP_WEIGHT, last)
        gather_forward(0, rf_full if last else rb_full)
        behind(1, STEP_WEIGHT, last)

    for c in range(CHAINS):
        rs_res[c] = y_tile[pl.ds(pl.multiple_of(c * half + my_tg * th, th), th), :]
    behind(0, 1.0, False)
    gather_forward(0, rb_full)
    behind(1, 1.0, False)
    lax.fori_loop(0, SWEEPS - 1, lambda s, _: (sweep(s, False), 0)[1], 0)
    sweep(SWEEPS - 1, True)
    gather_forward(1, rf_full)

    for c in range(CHAINS):
        gather_wait(c, rf_full)
    pltpu.make_async_copy(w_nat, w_out, out_sem.at[0]).wait()
    for g in range(n_sg):
        both = jnp.concatenate([rf_full[c, g * n_tg:(g + 1) * n_tg].reshape(half, TILE) for c in range(CHAINS)], axis=0)
        w_nat[g * TILE:(g + 1) * TILE, :] = both.T
    r_copy = pltpu.make_async_copy(w_nat, r_out, out_sem.at[1])
    r_copy.start()
    for c in range(CHAINS):
        gather_sent(c, rf_full)
    r_copy.wait()


def solution(mesh):
    n_samp, n_feat = mesh.shape["samp"], mesh.shape["feat"]
    side = round(n_feat ** (1 / 3))
    design_spec = P(("problem", "samp"), "feat")
    rows_spec = P(("problem", "samp"), None)
    coef_spec = P(("problem", "feat"), None)
    step_spec = P(("problem", "feat"))
    ridge_spec = P("problem")

    def local_sweeps(design, targets, coef_init, step_sizes, ridge_weights):
        rows, feats = design.shape
        tgt = targets.shape[1]
        half = tgt // CHAINS
        n_fb, n_sb = feats // BIG, rows // BIG
        n_tg = n_feat // (rows // TILE)
        th = half // n_tg
        f32, bf16 = jnp.float32, jnp.bfloat16
        hbm = pl.BlockSpec(memory_space=pl.ANY)
        vmem = pl.BlockSpec(memory_space=pltpu.VMEM)
        return pl.pallas_call(
            functools.partial(_kernel, side, n_feat, n_samp),
            name="descent",
            out_shape=(jax.ShapeDtypeStruct((feats, tgt), f32), jax.ShapeDtypeStruct((rows, tgt), f32)),
            in_specs=[hbm, hbm, hbm, vmem, vmem],
            out_specs=(hbm, hbm),
            scratch_shapes=[
                pltpu.VMEM((rows, feats), bf16),
                pltpu.VMEM((feats, rows), bf16),
                pltpu.VMEM((feats, tgt), f32),
                pltpu.VMEM((CHAINS, n_fb, half, BIG), f32),
                pltpu.VMEM((CHAINS, half, feats), bf16),
                pltpu.VMEM((CHAINS, n_feat, th, TILE), bf16),
                pltpu.VMEM((CHAINS, n_feat, th, TILE), bf16),
                pltpu.VMEM((CHAINS, n_feat, th, TILE), bf16),
                pltpu.VMEM((CHAINS, n_fb, half, BIG), f32),
                pltpu.VMEM((2, CHAINS, n_fb, half, BIG), f32),
                pltpu.VMEM((CHAINS, th, TILE), f32),
                pltpu.VMEM((CHAINS, n_feat, th, TILE), f32),
                pltpu.VMEM((TILE, tgt), f32),
                pltpu.VMEM((tgt, tgt), f32),
                pltpu.SemaphoreType.DMA((n_sb,)),
                pltpu.SemaphoreType.DMA((2,)),
                pltpu.SemaphoreType.DMA((CHAINS,)),
                pltpu.SemaphoreType.DMA((CHAINS,)),
                pltpu.SemaphoreType.DMA((CHAINS,)),
                pltpu.SemaphoreType.DMA((CHAINS, side * side)),
                pltpu.SemaphoreType.DMA((CHAINS,)),
                pltpu.SemaphoreType.DMA((CHAINS, n_fb)),
                pltpu.SemaphoreType.DMA((2, CHAINS, n_fb)),
                pltpu.SemaphoreType.DMA((2,)),
            ],
            compiler_params=pltpu.CompilerParams(collective_id=0, has_side_effects=True, vmem_limit_bytes=56 * 1024 * 1024),
        )(design, targets, coef_init, step_sizes[None, :], ridge_weights[None, :])

    return jax.shard_map(local_sweeps, mesh=mesh, in_specs=(design_spec, rows_spec, coef_spec, step_spec, ridge_spec), out_specs=(coef_spec, rows_spec), check_vma=False)
```

```python
import functools

import jax
import jax.numpy as jnp
from jax import lax
from jax.experimental import pallas as pl
from jax.experimental.pallas import tpu as pltpu
from jax.sharding import PartitionSpec as P

SWEEPS = 4
STEP_WEIGHT = 0.5
CHAINS = 2
TILE = 128
BIG = 512
MESH = pl.DeviceIdType.MESH


def _kernel(side, n_feat, n_samp, x_hbm, y_hbm, w0_hbm, eta_ref, lam_ref, w_out, r_out,
            x_v, xt_v, w_nat, w_t, st, u_buf, rs_recv, rb_full, gt, g_recv, rs_res, rf_full, y_tile, lam_t,
            x_sem, in_sem, rs_ssem, rs_rsem, ag_ssem, ag_psem, ag_rsem, g_ssem, g_rsem, out_sem):
    rows, feats = x_v.shape
    targets = w_nat.shape[1]
    half = targets // CHAINS
    n_sg = rows // TILE
    n_tg = n_feat // n_sg
    th = half // n_tg
    n_fb, n_sb = feats // BIG, rows // BIG

    def hops(*by):
        return sum(min(d, side - d) for d in by)

    steps = range(side)
    plane = sorted([(a, b) for a in steps for b in steps if a or b], key=lambda o: hops(*o))
    far_first = sorted([(a, b, d) for a in steps for b in steps for d in steps if a or b or d],
                       key=lambda o: (-hops(*o), (o[0] + 3 * o[1] + 5 * o[2]) % 7))
    per_sb = n_feat // n_sb
    total_rows = rows * n_samp

    me = lax.axis_index("feat")
    core = lax.axis_index("samp")

    barrier = pltpu.get_barrier_semaphore()

    def greet(d, _):
        pl.semaphore_signal(barrier, inc=1, device_id={"feat": (me + d) % n_feat}, device_id_type=MESH)
        return 0

    lax.fori_loop(1, n_feat, greet, 0)
    pl.semaphore_signal(barrier, inc=1, device_id={"samp": 1 - core}, device_id_type=MESH)

    w_load = pltpu.make_async_copy(w0_hbm, w_nat, in_sem.at[0])
    w_load.start()

    mz, my, mx = me // (side * side), (me // side) % side, me % side
    my_sb, my_in_sb = (mx + my + mz) % side, mz * side + my
    pos = my_sb * per_sb + my_in_sb

    def block_rows(k):
        return pl.ds(pl.multiple_of(((my_sb + k + 1) % n_sb) * BIG, BIG), BIG)

    def x_load(k):
        return pltpu.make_async_copy(x_hbm.at[block_rows(k)], x_v.at[block_rows(k)], x_sem.at[k])

    for k in range(n_sb):
        x_load(k).start()
    my_sg, my_tg = pos // n_tg, pos % n_tg
    y_load = pltpu.make_async_copy(y_hbm.at[pl.ds(pl.multiple_of(my_sg * TILE, TILE), TILE)], y_tile, in_sem.at[1])
    y_load.start()

    def rs_copy(c, place, peer):
        return pltpu.make_async_remote_copy(src_ref=u_buf.at[c, place], dst_ref=rs_recv.at[c, pos], send_sem=rs_ssem.at[c],
                                            recv_sem=rs_rsem.at[c], device_id={"feat": peer}, device_id_type=MESH)

    def rs_all(c):
        return pltpu.make_async_remote_copy(src_ref=u_buf.at[c, pl.ds(1, n_feat - 1)], dst_ref=rs_recv.at[c, pl.ds(1, n_feat - 1)],
                                            send_sem=rs_ssem.at[c], recv_sem=rs_rsem.at[c], device_id={"feat": me},
                                            device_id_type=MESH)

    def send_tiles(c, k, u):
        sb = (my_sb + k + 1) % n_sb

        def send(dz, dy, when):
            z, y = (mz + dz) % side, (my + dy) % side
            x = (sb + 2 * side - z - y) % side
            copy = rs_copy(c, sb * per_sb + z * side + y, z * side * side + y * side + x)
            if when is True:
                copy.start()
            else:
                pl.when(when)(copy.start)

        for j in range(per_sb):
            g, t = j // n_tg, j % n_tg
            u_buf[c, sb * per_sb + j] = u[t * th:(t + 1) * th, g * TILE:(g + 1) * TILE].astype(jnp.bfloat16)
        for a, b in reversed(plane):
            send(a, b, True)
        send(0, 0, k != n_sb - 1)

    def reduce(c, coef):
        rs_all(c).wait_recv()
        rs_recv[c, pos] = u_buf[c, pos]
        accs = [rs_recv[c, j].astype(jnp.float32) for j in range(4)]
        for j in range(4, n_feat):
            accs[j % 4] = accs[j % 4] + rs_recv[c, j].astype(jnp.float32)
        total = (accs[0] + accs[1]) + (accs[2] + accs[3])
        rs_res[c] = rs_res[c] - coef * total

    def place_of(device):
        z, y, x = device // (side * side), (device // side) % side, device % side
        return (x + y + z) % side * per_sb + z * side + y

    def axes(first_axis):
        kinds = (first_axis, (first_axis + 1) % 3, (first_axis + 2) % 3)
        strides = [jnp.where(d == 0, 1, jnp.where(d == 1, side, side * side)) for d in kinds]
        return [(stride, (me // stride) % side) for stride in strides]

    def moved(axis, by):
        stride, at = axis
        return ((at + by) % side - at) * stride

    def gather_copy(c, ref, place, peer, recv_sem):
        return pltpu.make_async_remote_copy(src_ref=ref.at[c, place], dst_ref=ref.at[c, place], send_sem=ag_ssem.at[c],
                                            recv_sem=recv_sem, device_id={"feat": peer}, device_id_type=MESH)

    def gather_start(c):
        moves = [[moved(axis, by) for by in range(side)] for axis in axes(core % 3)]
        for a, b, d in far_first:
            gather_copy(c, rb_full, pos, me + moves[0][a] + moves[1][b] + moves[2][d], ag_rsem.at[c]).start()

    def pass_on(c, place):
        ring = axes((c * n_samp + core) % 3)[0]
        for d in range(side - 1, 0, -1):
            gather_copy(c, rf_full, place, me + moved(ring, d), ag_rsem.at[c]).start()

    def last_gather_start(c):
        _, one, two = axes((c * n_samp + core) % 3)
        for i in range(len(plane) - 1, -1, -1):
            a, b = plane[i]
            gather_copy(c, rf_full, pos, me + moved(one, a) + moved(two, b), ag_psem.at[c, i]).start()
        pass_on(c, pos)

    def last_gather_forward(c):
        _, one, two = axes((c * n_samp + core) % 3)
        for i, (a, b) in enumerate(plane):
            place = place_of(me + moved(one, side - a) + moved(two, side - b))
            gather_copy(c, rf_full, place, me, ag_psem.at[c, i]).wait_recv()
            pass_on(c, place)

    def gather_wait(c, ref, tiles):
        part = ref.at[c, pl.ds(0, tiles)]
        pltpu.make_async_remote_copy(src_ref=part, dst_ref=part, send_sem=ag_ssem.at[c], recv_sem=ag_rsem.at[c],
                                     device_id={"feat": me}, device_id_type=MESH).wait_recv()

    def gather_sent(c, ref):
        part = ref.at[c, pl.ds(1, n_feat - 1)]
        pltpu.make_async_remote_copy(src_ref=part, dst_ref=part, send_sem=ag_ssem.at[c], recv_sem=ag_rsem.at[c],
                                     device_id={"feat": me}, device_id_type=MESH).wait_send()

    def g_copy(c, par, f):
        return pltpu.make_async_remote_copy(src_ref=gt.at[c, f], dst_ref=g_recv.at[par, c, f], send_sem=g_ssem.at[c, f],
                                            recv_sem=g_rsem.at[par, c, f], device_id={"samp": 1 - core}, device_id_type=MESH)

    w_load.wait()
    for f in range(n_fb):
        wt = w_nat[f * BIG:(f + 1) * BIG, :].T
        for c in range(CHAINS):
            w_t[c, f] = wt[c * half:(c + 1) * half]
            st[c, :, f * BIG:(f + 1) * BIG] = wt[c * half:(c + 1) * half].astype(jnp.bfloat16)
    lam_t[...] = jnp.broadcast_to(lam_ref[...], (targets, targets)).T
    x_load(0).wait()
    pl.semaphore_wait(barrier, n_feat)

    def first(k, _):
        @pl.when(k > 0)
        def _():
            x_load(k).wait()
        u = lax.dot_general(st[...].reshape(targets, feats), x_v[block_rows(k), :], (((1,), (1,)), ((), ())),
                            preferred_element_type=jnp.float32)
        for c in range(CHAINS):
            send_tiles(c, k, u[c * half:(c + 1) * half])
        return 0

    lax.fori_loop(0, n_sb, first, 0)

    def turn(r, _):
        piece = pl.ds(pl.multiple_of(r * TILE, TILE), TILE)
        xt_v[:, piece] = x_v[piece, :].T
        return 0

    lax.fori_loop(0, n_sg, turn, 0)
    y_load.wait()
    y_tile[...] = y_tile[...].T

    def behind(c, coef, last):
        reduce(c, coef)
        if last:
            rf_full[c, pos] = rs_res[c]
            last_gather_start(c)
        else:
            rb_full[c, pos] = rs_res[c].astype(jnp.bfloat16)
            gather_start(c)
        rs_all(c).wait_send()

    def gradient_part(c, par):
        gather_wait(c, rb_full, n_feat - 1)
        rbt = jnp.concatenate([rb_full[c, g * n_tg:(g + 1) * n_tg].reshape(half, TILE) for g in range(n_sg)], axis=1)

        def grad(f, _):
            cols = pl.ds(pl.multiple_of(f * BIG, BIG), BIG)
            gt[c, f] = jnp.dot(rbt, x_v[:, cols], preferred_element_type=jnp.float32)
            g_copy(c, par, f).start()
            return 0

        lax.fori_loop(0, n_fb, grad, 0)

    def step_and_product(c, par):
        lam = lam_t[c * half:(c + 1) * half, :]
        lam = jnp.concatenate([lam] * (BIG // targets), axis=1)

        def step(f, _):
            g_copy(c, par, f).wait_recv()
            cols = pl.ds(pl.multiple_of(f * BIG, BIG), BIG)
            gradient = (gt[c, f] + g_recv[par, c, f]) / total_rows
            w = w_t[c, f]
            delta = eta_ref[:, cols] * (gradient - lam * w)
            w_t[c, f] = w + STEP_WEIGHT * delta
            st[c, :, cols] = delta.astype(jnp.bfloat16)
            return 0

        lax.fori_loop(0, n_fb, step, 0)
        gather_sent(c, rb_full)

        def product(k, _):
            send_tiles(c, k, jnp.dot(st[c], xt_v[:, block_rows(k)], preferred_element_type=jnp.float32))
            return 0

        lax.fori_loop(0, n_sb, product, 0)
        for f in range(n_fb):
            g_copy(c, par, f).wait_send()

    def sweep(s, last):
        par = s % 2
        gradient_part(0, par)
        behind(1, jnp.where(s == 0, 1.0, STEP_WEIGHT), False)
        step_and_product(0, par)
        gradient_part(1, par)
        behind(0, STEP_WEIGHT, last)
        step_and_product(1, par)
        if last:
            for f in range(n_fb):
                w_nat[f * BIG:(f + 1) * BIG, :] = jnp.concatenate([w_t[c, f] for c in range(CHAINS)], axis=0).T
            pltpu.make_async_copy(w_nat, w_out, out_sem.at[0]).start()
            last_gather_forward(0)
            behind(1, STEP_WEIGHT, True)
            last_gather_forward(1)

    for c in range(CHAINS):
        rs_res[c] = y_tile[pl.ds(pl.multiple_of(c * half + my_tg * th, th), th), :]
    behind(0, 1.0, False)
    lax.fori_loop(0, SWEEPS - 1, lambda s, _: (sweep(s, False), 0)[1], 0)
    sweep(SWEEPS - 1, True)

    for c in range(CHAINS):
        gather_wait(c, rf_full, n_feat - side * side)
    pltpu.make_async_copy(w_nat, w_out, out_sem.at[0]).wait()
    for g in range(n_sg):
        both = jnp.concatenate([rf_full[c, g * n_tg:(g + 1) * n_tg].reshape(half, TILE) for c in range(CHAINS)], axis=0)
        w_nat[g * TILE:(g + 1) * TILE, :] = both.T
    r_copy = pltpu.make_async_copy(w_nat, r_out, out_sem.at[1])
    r_copy.start()
    for c in range(CHAINS):
        gather_sent(c, rf_full)
    r_copy.wait()


def solution(mesh):
    n_samp, n_feat = mesh.shape["samp"], mesh.shape["feat"]
    side = round(n_feat ** (1 / 3))
    design_spec = P(("problem", "samp"), "feat")
    rows_spec = P(("problem", "samp"), None)
    coef_spec = P(("problem", "feat"), None)
    step_spec = P(("problem", "feat"))
    ridge_spec = P("problem")

    def local_sweeps(design, targets, coef_init, step_sizes, ridge_weights):
        rows, feats = design.shape
        tgt = targets.shape[1]
        half = tgt // CHAINS
        n_fb, n_sb = feats // BIG, rows // BIG
        n_tg = n_feat // (rows // TILE)
        th = half // n_tg
        f32, bf16 = jnp.float32, jnp.bfloat16
        hbm = pl.BlockSpec(memory_space=pl.ANY)
        vmem = pl.BlockSpec(memory_space=pltpu.VMEM)
        return pl.pallas_call(
            functools.partial(_kernel, side, n_feat, n_samp),
            name="descent",
            out_shape=(jax.ShapeDtypeStruct((feats, tgt), f32), jax.ShapeDtypeStruct((rows, tgt), f32)),
            in_specs=[hbm, hbm, hbm, vmem, vmem],
            out_specs=(hbm, hbm),
            scratch_shapes=[
                pltpu.VMEM((rows, feats), bf16),
                pltpu.VMEM((feats, rows), bf16),
                pltpu.VMEM((feats, tgt), f32),
                pltpu.VMEM((CHAINS, n_fb, half, BIG), f32),
                pltpu.VMEM((CHAINS, half, feats), bf16),
                pltpu.VMEM((CHAINS, n_feat, th, TILE), bf16),
                pltpu.VMEM((CHAINS, n_feat, th, TILE), bf16),
                pltpu.VMEM((CHAINS, n_feat, th, TILE), bf16),
                pltpu.VMEM((CHAINS, n_fb, half, BIG), f32),
                pltpu.VMEM((2, CHAINS, n_fb, half, BIG), f32),
                pltpu.VMEM((CHAINS, th, TILE), f32),
                pltpu.VMEM((CHAINS, n_feat, th, TILE), f32),
                pltpu.VMEM((TILE, tgt), f32),
                pltpu.VMEM((tgt, tgt), f32),
                pltpu.SemaphoreType.DMA((n_sb,)),
                pltpu.SemaphoreType.DMA((2,)),
                pltpu.SemaphoreType.DMA((CHAINS,)),
                pltpu.SemaphoreType.DMA((CHAINS,)),
                pltpu.SemaphoreType.DMA((CHAINS,)),
                pltpu.SemaphoreType.DMA((CHAINS, side * side)),
                pltpu.SemaphoreType.DMA((CHAINS,)),
                pltpu.SemaphoreType.DMA((CHAINS, n_fb)),
                pltpu.SemaphoreType.DMA((2, CHAINS, n_fb)),
                pltpu.SemaphoreType.DMA((2,)),
            ],
            compiler_params=pltpu.CompilerParams(collective_id=0, has_side_effects=True, vmem_limit_bytes=56 * 1024 * 1024),
        )(design, targets, coef_init, step_sizes[None, :], ridge_weights[None, :])

    return jax.shard_map(local_sweeps, mesh=mesh, in_specs=(design_spec, rows_spec, coef_spec, step_spec, ridge_spec), out_specs=(coef_spec, rows_spec), check_vma=False)
```

```python
import functools

import jax
import jax.numpy as jnp
from jax import lax
from jax.experimental import pallas as pl
from jax.experimental.pallas import tpu as pltpu
from jax.sharding import PartitionSpec as P

SWEEPS = 4
STEP_WEIGHT = 0.5
CHAINS = 2
TILE = 128
BIG = 512
MXU = 256
MESH = pl.DeviceIdType.MESH


def _kernel(side, n_feat, n_samp, x_hbm, y_hbm, w0_hbm, eta_ref, lam_ref, w_out, r_out,
            x_v, xt_v, w_nat, w_t, st, u_buf, rs_recv, rb_full, gt, g_recv, rs_res, rf_full, y_tile, lam_t,
            x_sem, in_sem, rs_ssem, rs_rsem, ag_ssem, ag_psem, ag_rsem, g_ssem, g_rsem):
    rows, feats = x_v.shape
    targets = w_nat.shape[1]
    half = targets // CHAINS
    n_sg = rows // TILE
    n_tg = n_feat // n_sg
    th = half // n_tg
    n_fb, n_sb = feats // BIG, rows // BIG

    def hops(*by):
        return sum(min(d, side - d) for d in by)

    steps = range(side)
    plane = sorted([(a, b) for a in steps for b in steps if a or b], key=lambda o: hops(*o))
    far_first = sorted([(a, b, d) for a in steps for b in steps for d in steps if a or b or d],
                       key=lambda o: (-hops(*o), (o[0] + 3 * o[1] + 5 * o[2]) % 7))
    per_sb = n_feat // n_sb
    total_rows = rows * n_samp

    me = lax.axis_index("feat")
    core = lax.axis_index("samp")

    barrier = pltpu.get_barrier_semaphore()

    def greet(d, _):
        pl.semaphore_signal(barrier, inc=1, device_id={"feat": (me + d) % n_feat}, device_id_type=MESH)
        return 0

    lax.fori_loop(1, n_feat, greet, 0)
    pl.semaphore_signal(barrier, inc=1, device_id={"samp": 1 - core}, device_id_type=MESH)

    w_load = pltpu.make_async_copy(w0_hbm, w_nat, in_sem.at[0])
    w_load.start()

    mz, my, mx = me // (side * side), (me // side) % side, me % side
    my_sb, my_in_sb = (mx + my + mz) % side, mz * side + my
    pos = my_sb * per_sb + my_in_sb

    def block_rows(k):
        return pl.ds(pl.multiple_of(((my_sb + k + 1) % n_sb) * BIG, BIG), BIG)

    def x_load(k):
        return pltpu.make_async_copy(x_hbm.at[block_rows(k)], x_v.at[block_rows(k)], x_sem.at[k])

    for k in range(n_sb):
        x_load(k).start()
    my_sg, my_tg = pos // n_tg, pos % n_tg
    y_load = pltpu.make_async_copy(y_hbm.at[pl.ds(pl.multiple_of(my_sg * TILE, TILE), TILE)], y_tile, in_sem.at[1])
    y_load.start()

    def rs_copy(c, place, peer):
        return pltpu.make_async_remote_copy(src_ref=u_buf.at[c, place], dst_ref=rs_recv.at[c, pos], send_sem=rs_ssem.at[c],
                                            recv_sem=rs_rsem.at[c], device_id={"feat": peer}, device_id_type=MESH)

    def rs_all(c):
        return pltpu.make_async_remote_copy(src_ref=u_buf.at[c, pl.ds(1, n_feat - 1)], dst_ref=rs_recv.at[c, pl.ds(1, n_feat - 1)],
                                            send_sem=rs_ssem.at[c], recv_sem=rs_rsem.at[c], device_id={"feat": me},
                                            device_id_type=MESH)

    def send_tiles(c, k, u):
        sb = (my_sb + k + 1) % n_sb

        def send(dz, dy, when):
            z, y = (mz + dz) % side, (my + dy) % side
            x = (sb + 2 * side - z - y) % side
            copy = rs_copy(c, sb * per_sb + z * side + y, z * side * side + y * side + x)
            if when is True:
                copy.start()
            else:
                pl.when(when)(copy.start)

        for j in range(per_sb):
            g, t = j // n_tg, j % n_tg
            u_buf[c, sb * per_sb + j] = u[t * th:(t + 1) * th, g * TILE:(g + 1) * TILE].astype(jnp.bfloat16)
        for a, b in reversed(plane):
            send(a, b, True)
        send(0, 0, k != n_sb - 1)

    def reduce(c, coef):
        rs_all(c).wait_recv()
        rs_recv[c, pos] = u_buf[c, pos]
        accs = [rs_recv[c, j].astype(jnp.float32) for j in range(4)]
        for j in range(4, n_feat):
            accs[j % 4] = accs[j % 4] + rs_recv[c, j].astype(jnp.float32)
        total = (accs[0] + accs[1]) + (accs[2] + accs[3])
        rs_res[c] = rs_res[c] - coef * total

    def place_of(device):
        z, y, x = device // (side * side), (device // side) % side, device % side
        return (x + y + z) % side * per_sb + z * side + y

    def axes(first_axis):
        kinds = (first_axis, (first_axis + 1) % 3, (first_axis + 2) % 3)
        strides = [jnp.where(d == 0, 1, jnp.where(d == 1, side, side * side)) for d in kinds]
        return [(stride, (me // stride) % side) for stride in strides]

    def moved(axis, by):
        stride, at = axis
        return ((at + by) % side - at) * stride

    def gather_copy(c, ref, place, peer, recv_sem):
        return pltpu.make_async_remote_copy(src_ref=ref.at[c, place], dst_ref=ref.at[c, place], send_sem=ag_ssem.at[c],
                                            recv_sem=recv_sem, device_id={"feat": peer}, device_id_type=MESH)

    def gather_start(c):
        moves = [[moved(axis, by) for by in range(side)] for axis in axes(core % 3)]
        for a, b, d in far_first:
            gather_copy(c, rb_full, pos, me + moves[0][a] + moves[1][b] + moves[2][d], ag_rsem.at[c]).start()

    def pass_on(c, place):
        ring = axes((c * n_samp + core) % 3)[0]
        for d in range(side - 1, 0, -1):
            gather_copy(c, rf_full, place, me + moved(ring, d), ag_rsem.at[c]).start()

    def last_gather_start(c):
        _, one, two = axes((c * n_samp + core) % 3)
        for i in range(len(plane) - 1, -1, -1):
            a, b = plane[i]
            gather_copy(c, rf_full, pos, me + moved(one, a) + moved(two, b), ag_psem.at[c, i]).start()
        pass_on(c, pos)

    def last_gather_forward(c):
        _, one, two = axes((c * n_samp + core) % 3)
        for i, (a, b) in enumerate(plane):
            place = place_of(me + moved(one, side - a) + moved(two, side - b))
            gather_copy(c, rf_full, place, me, ag_psem.at[c, i]).wait_recv()
            pass_on(c, place)

    def gather_wait(c, ref, tiles):
        part = ref.at[c, pl.ds(0, tiles)]
        pltpu.make_async_remote_copy(src_ref=part, dst_ref=part, send_sem=ag_ssem.at[c], recv_sem=ag_rsem.at[c],
                                     device_id={"feat": me}, device_id_type=MESH).wait_recv()

    def gather_sent(c, ref):
        part = ref.at[c, pl.ds(1, n_feat - 1)]
        pltpu.make_async_remote_copy(src_ref=part, dst_ref=part, send_sem=ag_ssem.at[c], recv_sem=ag_rsem.at[c],
                                     device_id={"feat": me}, device_id_type=MESH).wait_send()

    def g_copy(c, par, f):
        return pltpu.make_async_remote_copy(src_ref=gt.at[c, f], dst_ref=g_recv.at[par, c, f], send_sem=g_ssem.at[c, f],
                                            recv_sem=g_rsem.at[par, c, f], device_id={"samp": 1 - core}, device_id_type=MESH)

    w_load.wait()
    for f in range(n_fb):
        wt = w_nat[f * BIG:(f + 1) * BIG, :].T
        for c in range(CHAINS):
            w_t[c, f] = wt[c * half:(c + 1) * half]
            st[c, :, f * BIG:(f + 1) * BIG] = wt[c * half:(c + 1) * half].astype(jnp.bfloat16)
    lam_t[...] = jnp.broadcast_to(lam_ref[...], (targets, targets)).T
    x_load(0).wait()
    pl.semaphore_wait(barrier, n_feat)

    def first(k, _):
        @pl.when(k > 0)
        def _():
            x_load(k).wait()
        u = lax.dot_general(st[...].reshape(targets, feats), x_v[block_rows(k), :], (((1,), (1,)), ((), ())),
                            preferred_element_type=jnp.float32)
        for c in range(CHAINS):
            send_tiles(c, k, u[c * half:(c + 1) * half])
        return 0

    lax.fori_loop(0, n_sb, first, 0)

    eye = (lax.broadcasted_iota(jnp.int32, (MXU, MXU), 0) == lax.broadcasted_iota(jnp.int32, (MXU, MXU), 1)).astype(jnp.bfloat16)

    def turn(r, _):
        piece = pl.ds(pl.multiple_of(r * MXU, MXU), MXU)
        for f in range(0, feats, MXU):
            turned = lax.dot_general(eye, x_v[piece, f:f + MXU], (((1,), (1,)), ((), ())), preferred_element_type=jnp.float32)
            xt_v[f:f + MXU, piece] = turned.astype(jnp.bfloat16)
        return 0

    lax.fori_loop(0, rows // MXU // 2, turn, 0)
    y_load.wait()
    y_tile[...] = y_tile[...].T

    def behind(c, coef, last):
        reduce(c, coef)
        if last:
            rf_full[c, pos] = rs_res[c]
            last_gather_start(c)
        else:
            rb_full[c, pos] = rs_res[c].astype(jnp.bfloat16)
            gather_start(c)
        rs_all(c).wait_send()

    def gradient_part(c, par):
        gather_wait(c, rb_full, n_feat - 1)
        rbt = jnp.concatenate([rb_full[c, g * n_tg:(g + 1) * n_tg].reshape(half, TILE) for g in range(n_sg)], axis=1)

        def grad(f, _):
            cols = pl.ds(pl.multiple_of(f * BIG, BIG), BIG)
            gt[c, f] = jnp.dot(rbt, x_v[:, cols], preferred_element_type=jnp.float32)
            g_copy(c, par, f).start()
            return 0

        lax.fori_loop(0, n_fb, grad, 0)

    def step_and_product(c, par):
        lam = lam_t[c * half:(c + 1) * half, :]
        lam = jnp.concatenate([lam] * (BIG // targets), axis=1)

        def step(f, _):
            g_copy(c, par, f).wait_recv()
            cols = pl.ds(pl.multiple_of(f * BIG, BIG), BIG)
            gradient = (gt[c, f] + g_recv[par, c, f]) / total_rows
            w = w_t[c, f]
            delta = eta_ref[:, cols] * (gradient - lam * w)
            w_t[c, f] = w + STEP_WEIGHT * delta
            st[c, :, cols] = delta.astype(jnp.bfloat16)
            return 0

        lax.fori_loop(0, n_fb, step, 0)
        gather_sent(c, rb_full)

        def product(k, _):
            send_tiles(c, k, jnp.dot(st[c], xt_v[:, block_rows(k)], preferred_element_type=jnp.float32))
            return 0

        lax.fori_loop(0, n_sb, product, 0)
        for f in range(n_fb):
            g_copy(c, par, f).wait_send()

    def sweep(s, last):
        par = s % 2
        gradient_part(0, par)
        behind(1, jnp.where(s == 0, 1.0, STEP_WEIGHT), False)
        step_and_product(0, par)
        gradient_part(1, par)
        behind(0, STEP_WEIGHT, last)
        step_and_product(1, par)
        if last:
            for f in range(n_fb):
                w_out[f * BIG:(f + 1) * BIG, :] = jnp.concatenate([w_t[c, f] for c in range(CHAINS)], axis=0).T
            last_gather_forward(0)
            behind(1, STEP_WEIGHT, True)
            last_gather_forward(1)

    for c in range(CHAINS):
        rs_res[c] = y_tile[pl.ds(pl.multiple_of(c * half + my_tg * th, th), th), :]
    behind(0, 1.0, False)
    lax.fori_loop(rows // MXU // 2, rows // MXU, turn, 0)
    lax.fori_loop(0, SWEEPS - 1, lambda s, _: (sweep(s, False), 0)[1], 0)
    sweep(SWEEPS - 1, True)

    for c in range(CHAINS):
        gather_wait(c, rf_full, n_feat - side * side)
    for g in range(n_sg):
        both = jnp.concatenate([rf_full[c, g * n_tg:(g + 1) * n_tg].reshape(half, TILE) for c in range(CHAINS)], axis=0)
        r_out[g * TILE:(g + 1) * TILE, :] = both.T
    for c in range(CHAINS):
        gather_sent(c, rf_full)


def _write(w_ref, r_ref, w_out, r_out, sem):
    copies = [pltpu.make_async_copy(w_ref, w_out, sem.at[0]), pltpu.make_async_copy(r_ref, r_out, sem.at[1])]
    for copy in copies:
        copy.start()
    for copy in copies:
        copy.wait()


def solution(mesh):
    n_samp, n_feat = mesh.shape["samp"], mesh.shape["feat"]
    side = round(n_feat ** (1 / 3))
    design_spec = P(("problem", "samp"), "feat")
    rows_spec = P(("problem", "samp"), None)
    coef_spec = P(("problem", "feat"), None)
    step_spec = P(("problem", "feat"))
    ridge_spec = P("problem")

    def local_sweeps(design, targets, coef_init, step_sizes, ridge_weights):
        rows, feats = design.shape
        tgt = targets.shape[1]
        half = tgt // CHAINS
        n_fb, n_sb = feats // BIG, rows // BIG
        n_tg = n_feat // (rows // TILE)
        th = half // n_tg
        f32, bf16 = jnp.float32, jnp.bfloat16
        hbm = pl.BlockSpec(memory_space=pl.ANY)
        vmem = pl.BlockSpec(memory_space=pltpu.VMEM)
        w, r = pl.pallas_call(
            functools.partial(_kernel, side, n_feat, n_samp),
            name="descent",
            out_shape=(pltpu.VMEM((feats, tgt), f32), pltpu.VMEM((rows, tgt), f32)),
            in_specs=[hbm, hbm, hbm, vmem, vmem],
            out_specs=(vmem, vmem),
            scratch_shapes=[
                pltpu.VMEM((rows, feats), bf16),
                pltpu.VMEM((feats, rows), bf16),
                pltpu.VMEM((feats, tgt), f32),
                pltpu.VMEM((CHAINS, n_fb, half, BIG), f32),
                pltpu.VMEM((CHAINS, half, feats), bf16),
                pltpu.VMEM((CHAINS, n_feat, th, TILE), bf16),
                pltpu.VMEM((CHAINS, n_feat, th, TILE), bf16),
                pltpu.VMEM((CHAINS, n_feat, th, TILE), bf16),
                pltpu.VMEM((CHAINS, n_fb, half, BIG), f32),
                pltpu.VMEM((2, CHAINS, n_fb, half, BIG), f32),
                pltpu.VMEM((CHAINS, th, TILE), f32),
                pltpu.VMEM((CHAINS, n_feat, th, TILE), f32),
                pltpu.VMEM((TILE, tgt), f32),
                pltpu.VMEM((tgt, tgt), f32),
                pltpu.SemaphoreType.DMA((n_sb,)),
                pltpu.SemaphoreType.DMA((2,)),
                pltpu.SemaphoreType.DMA((CHAINS,)),
                pltpu.SemaphoreType.DMA((CHAINS,)),
                pltpu.SemaphoreType.DMA((CHAINS,)),
                pltpu.SemaphoreType.DMA((CHAINS, side * side)),
                pltpu.SemaphoreType.DMA((CHAINS,)),
                pltpu.SemaphoreType.DMA((CHAINS, n_fb)),
                pltpu.SemaphoreType.DMA((2, CHAINS, n_fb)),
            ],
            compiler_params=pltpu.CompilerParams(collective_id=0, has_side_effects=True, vmem_limit_bytes=56 * 1024 * 1024),
        )(design, targets, coef_init, step_sizes[None, :], ridge_weights[None, :])
        return pl.pallas_call(
            _write,
            name="write",
            out_shape=(jax.ShapeDtypeStruct(w.shape, f32), jax.ShapeDtypeStruct(r.shape, f32)),
            in_specs=[vmem, vmem],
            out_specs=(hbm, hbm),
            scratch_shapes=[pltpu.SemaphoreType.DMA((2,))],
        )(pltpu.with_memory_space_constraint(w, pltpu.VMEM), pltpu.with_memory_space_constraint(r, pltpu.VMEM))

    return jax.shard_map(local_sweeps, mesh=mesh, in_specs=(design_spec, rows_spec, coef_spec, step_spec, ridge_spec), out_specs=(coef_spec, rows_spec), check_vma=False)
```

```python
import functools

import jax
import jax.numpy as jnp
from jax import lax
from jax.experimental import pallas as pl
from jax.experimental.pallas import tpu as pltpu
from jax.sharding import PartitionSpec as P

SWEEPS = 4
STEP_WEIGHT = 0.5
CHAINS = 2
TILE = 128
BIG = 512
MXU = 256
MESH = pl.DeviceIdType.MESH


def _kernel(side, n_feat, n_samp, x_hbm, y_hbm, w0_hbm, eta_ref, lam_ref, w_out, r_out,
            x_v, xt_v, w_nat, w_t, st, u_buf, rs_recv, rb_full, gt, g_recv, rs_res, rf_full, y_tile, lam_t,
            x_sem, in_sem, rs_ssem, rs_rsem, ag_ssem, ag_psem, ag_rsem, g_ssem, g_rsem):
    rows, feats = x_v.shape
    targets = w_nat.shape[1]
    half = targets // CHAINS
    n_sg = rows // TILE
    n_tg = n_feat // n_sg
    th = half // n_tg
    n_fb, n_sb = feats // BIG, rows // BIG

    def hops(*by):
        return sum(min(d, side - d) for d in by)

    steps = range(side)
    plane = sorted([(a, b) for a in steps for b in steps if a or b], key=lambda o: hops(*o))
    far_first = sorted([(a, b, d) for a in steps for b in steps for d in steps if a or b or d],
                       key=lambda o: (-hops(*o), (o[0] + 3 * o[1] + 5 * o[2]) % 7))
    per_sb = n_feat // n_sb
    total_rows = rows * n_samp

    me = lax.axis_index("feat")
    core = lax.axis_index("samp")

    barrier = pltpu.get_barrier_semaphore()

    def greet(d, _):
        pl.semaphore_signal(barrier, inc=1, device_id={"feat": (me + d) % n_feat}, device_id_type=MESH)
        return 0

    lax.fori_loop(1, n_feat, greet, 0)
    pl.semaphore_signal(barrier, inc=1, device_id={"samp": 1 - core}, device_id_type=MESH)

    w_load = pltpu.make_async_copy(w0_hbm, w_nat, in_sem.at[0])
    w_load.start()

    mz, my, mx = me // (side * side), (me // side) % side, me % side
    my_sb, my_in_sb = (mx + my + mz) % side, mz * side + my
    pos = my_sb * per_sb + my_in_sb

    def block_rows(k):
        return pl.ds(pl.multiple_of(((my_sb + k + 1) % n_sb) * BIG, BIG), BIG)

    def x_load(k):
        return pltpu.make_async_copy(x_hbm.at[block_rows(k)], x_v.at[block_rows(k)], x_sem.at[k])

    for k in range(n_sb):
        x_load(k).start()
    my_sg, my_tg = pos // n_tg, pos % n_tg
    y_load = pltpu.make_async_copy(y_hbm.at[pl.ds(pl.multiple_of(my_sg * TILE, TILE), TILE)], y_tile, in_sem.at[1])
    y_load.start()

    def rs_copy(c, place, peer):
        return pltpu.make_async_remote_copy(src_ref=u_buf.at[c, place], dst_ref=rs_recv.at[c, pos], send_sem=rs_ssem.at[c],
                                            recv_sem=rs_rsem.at[c], device_id={"feat": peer}, device_id_type=MESH)

    def rs_all(c):
        return pltpu.make_async_remote_copy(src_ref=u_buf.at[c, pl.ds(1, n_feat - 1)], dst_ref=rs_recv.at[c, pl.ds(1, n_feat - 1)],
                                            send_sem=rs_ssem.at[c], recv_sem=rs_rsem.at[c], device_id={"feat": me},
                                            device_id_type=MESH)

    def keep_tiles(c, k, u):
        sb = (my_sb + k + 1) % n_sb
        for j in range(per_sb):
            g, t = j // n_tg, j % n_tg
            u_buf[c, sb * per_sb + j] = u[t * th:(t + 1) * th, g * TILE:(g + 1) * TILE].astype(jnp.bfloat16)

    def send_tiles(c, k):
        sb = (my_sb + k + 1) % n_sb

        def send(dz, dy, when):
            z, y = (mz + dz) % side, (my + dy) % side
            x = (sb + 2 * side - z - y) % side
            copy = rs_copy(c, sb * per_sb + z * side + y, z * side * side + y * side + x)
            if when is True:
                copy.start()
            else:
                pl.when(when)(copy.start)

        for a, b in reversed(plane):
            send(a, b, True)
        send(0, 0, k != n_sb - 1)

    def reduce(c, coef):
        rs_all(c).wait_recv()
        rs_recv[c, pos] = u_buf[c, pos]
        accs = [rs_recv[c, j].astype(jnp.float32) for j in range(4)]
        for j in range(4, n_feat):
            accs[j % 4] = accs[j % 4] + rs_recv[c, j].astype(jnp.float32)
        total = (accs[0] + accs[1]) + (accs[2] + accs[3])
        rs_res[c] = rs_res[c] - coef * total

    def place_of(device):
        z, y, x = device // (side * side), (device // side) % side, device % side
        return (x + y + z) % side * per_sb + z * side + y

    def axes(first_axis):
        kinds = (first_axis, (first_axis + 1) % 3, (first_axis + 2) % 3)
        strides = [jnp.where(d == 0, 1, jnp.where(d == 1, side, side * side)) for d in kinds]
        return [(stride, (me // stride) % side) for stride in strides]

    def moved(axis, by):
        stride, at = axis
        return ((at + by) % side - at) * stride

    def gather_copy(c, ref, place, peer, recv_sem):
        return pltpu.make_async_remote_copy(src_ref=ref.at[c, place], dst_ref=ref.at[c, place], send_sem=ag_ssem.at[c],
                                            recv_sem=recv_sem, device_id={"feat": peer}, device_id_type=MESH)

    def gather_start(c):
        moves = [[moved(axis, by) for by in range(side)] for axis in axes(core % 3)]
        for a, b, d in far_first:
            gather_copy(c, rb_full, pos, me + moves[0][a] + moves[1][b] + moves[2][d], ag_rsem.at[c]).start()

    def pass_on(c, place):
        ring = axes((c * n_samp + core) % 3)[0]
        for d in range(side - 1, 0, -1):
            gather_copy(c, rf_full, place, me + moved(ring, d), ag_rsem.at[c]).start()

    def last_gather_start(c):
        _, one, two = axes((c * n_samp + core) % 3)
        for i in range(len(plane) - 1, -1, -1):
            a, b = plane[i]
            gather_copy(c, rf_full, pos, me + moved(one, a) + moved(two, b), ag_psem.at[c, i]).start()
        pass_on(c, pos)

    def last_gather_forward(c):
        _, one, two = axes((c * n_samp + core) % 3)
        for i, (a, b) in enumerate(plane):
            place = place_of(me + moved(one, side - a) + moved(two, side - b))
            gather_copy(c, rf_full, place, me, ag_psem.at[c, i]).wait_recv()
            pass_on(c, place)

    def gather_wait(c, ref, tiles):
        part = ref.at[c, pl.ds(0, tiles)]
        pltpu.make_async_remote_copy(src_ref=part, dst_ref=part, send_sem=ag_ssem.at[c], recv_sem=ag_rsem.at[c],
                                     device_id={"feat": me}, device_id_type=MESH).wait_recv()

    def gather_sent(c, ref):
        part = ref.at[c, pl.ds(1, n_feat - 1)]
        pltpu.make_async_remote_copy(src_ref=part, dst_ref=part, send_sem=ag_ssem.at[c], recv_sem=ag_rsem.at[c],
                                     device_id={"feat": me}, device_id_type=MESH).wait_send()

    def g_copy(c, par, f):
        return pltpu.make_async_remote_copy(src_ref=gt.at[c, f], dst_ref=g_recv.at[par, c, f], send_sem=g_ssem.at[c, f],
                                            recv_sem=g_rsem.at[par, c, f], device_id={"samp": 1 - core}, device_id_type=MESH)

    w_load.wait()
    for f in range(n_fb):
        wt = w_nat[f * BIG:(f + 1) * BIG, :].T
        for c in range(CHAINS):
            w_t[c, f] = wt[c * half:(c + 1) * half]
            st[c, :, f * BIG:(f + 1) * BIG] = wt[c * half:(c + 1) * half].astype(jnp.bfloat16)
    lam_t[...] = jnp.broadcast_to(lam_ref[...], (targets, targets)).T
    x_load(0).wait()
    pl.semaphore_wait(barrier, n_feat)

    def first(k, _):
        @pl.when(k > 0)
        def _():
            x_load(k).wait()
        u = lax.dot_general(st[...].reshape(targets, feats), x_v[block_rows(k), :], (((1,), (1,)), ((), ())),
                            preferred_element_type=jnp.float32)
        for c in range(CHAINS):
            keep_tiles(c, k, u[c * half:(c + 1) * half])
        send_tiles(0, k)
        return 0

    lax.fori_loop(0, n_sb, first, 0)
    lax.fori_loop(0, n_sb, lambda k, _: (send_tiles(1, k), 0)[1], 0)

    eye = (lax.broadcasted_iota(jnp.int32, (MXU, MXU), 0) == lax.broadcasted_iota(jnp.int32, (MXU, MXU), 1)).astype(jnp.bfloat16)

    def turn(r, _):
        piece = pl.ds(pl.multiple_of(r * MXU, MXU), MXU)
        for f in range(0, feats, MXU):
            turned = lax.dot_general(eye, x_v[piece, f:f + MXU], (((1,), (1,)), ((), ())), preferred_element_type=jnp.float32)
            xt_v[f:f + MXU, piece] = turned.astype(jnp.bfloat16)
        return 0

    lax.fori_loop(0, rows // MXU // 2, turn, 0)
    y_load.wait()
    y_tile[...] = y_tile[...].T

    def behind(c, coef, last):
        reduce(c, coef)
        if last:
            rf_full[c, pos] = rs_res[c]
            last_gather_start(c)
        else:
            rb_full[c, pos] = rs_res[c].astype(jnp.bfloat16)
            gather_start(c)
        rs_all(c).wait_send()

    def gradient_part(c, par):
        gather_wait(c, rb_full, n_feat - 1)
        rbt = jnp.concatenate([rb_full[c, g * n_tg:(g + 1) * n_tg].reshape(half, TILE) for g in range(n_sg)], axis=1)

        def grad(f, _):
            cols = pl.ds(pl.multiple_of(f * BIG, BIG), BIG)
            gt[c, f] = jnp.dot(rbt, x_v[:, cols], preferred_element_type=jnp.float32)
            g_copy(c, par, f).start()
            return 0

        lax.fori_loop(0, n_fb, grad, 0)

    def step_and_product(c, par):
        lam = lam_t[c * half:(c + 1) * half, :]
        lam = jnp.concatenate([lam] * (BIG // targets), axis=1)

        def step(f, _):
            g_copy(c, par, f).wait_recv()
            cols = pl.ds(pl.multiple_of(f * BIG, BIG), BIG)
            gradient = (gt[c, f] + g_recv[par, c, f]) / total_rows
            w = w_t[c, f]
            delta = eta_ref[:, cols] * (gradient - lam * w)
            w_t[c, f] = w + STEP_WEIGHT * delta
            st[c, :, cols] = delta.astype(jnp.bfloat16)
            return 0

        lax.fori_loop(0, n_fb, step, 0)
        gather_sent(c, rb_full)

        def product(k, _):
            keep_tiles(c, k, jnp.dot(st[c], xt_v[:, block_rows(k)], preferred_element_type=jnp.float32))
            send_tiles(c, k)
            return 0

        lax.fori_loop(0, n_sb, product, 0)
        for f in range(n_fb):
            g_copy(c, par, f).wait_send()

    def sweep(s, last):
        par = s % 2
        for c in range(CHAINS):
            gradient_part(c, par)
        for c in range(CHAINS):
            step_and_product(c, par)
        if last:
            for f in range(n_fb):
                w_out[f * BIG:(f + 1) * BIG, :] = jnp.concatenate([w_t[c, f] for c in range(CHAINS)], axis=0).T
        for c in range(CHAINS):
            behind(c, STEP_WEIGHT, last)

    for c in range(CHAINS):
        rs_res[c] = y_tile[pl.ds(pl.multiple_of(c * half + my_tg * th, th), th), :]
    for c in range(CHAINS):
        behind(c, 1.0, False)
    lax.fori_loop(rows // MXU // 2, rows // MXU, turn, 0)
    lax.fori_loop(0, SWEEPS - 1, lambda s, _: (sweep(s, False), 0)[1], 0)
    sweep(SWEEPS - 1, True)
    for c in range(CHAINS):
        last_gather_forward(c)

    for c in range(CHAINS):
        gather_wait(c, rf_full, n_feat - side * side)
    for g in range(n_sg):
        both = jnp.concatenate([rf_full[c, g * n_tg:(g + 1) * n_tg].reshape(half, TILE) for c in range(CHAINS)], axis=0)
        r_out[g * TILE:(g + 1) * TILE, :] = both.T
    for c in range(CHAINS):
        gather_sent(c, rf_full)


def _write(w_ref, r_ref, w_out, r_out, sem):
    copies = [pltpu.make_async_copy(w_ref, w_out, sem.at[0]), pltpu.make_async_copy(r_ref, r_out, sem.at[1])]
    for copy in copies:
        copy.start()
    for copy in copies:
        copy.wait()


def solution(mesh):
    n_samp, n_feat = mesh.shape["samp"], mesh.shape["feat"]
    side = round(n_feat ** (1 / 3))
    design_spec = P(("problem", "samp"), "feat")
    rows_spec = P(("problem", "samp"), None)
    coef_spec = P(("problem", "feat"), None)
    step_spec = P(("problem", "feat"))
    ridge_spec = P("problem")

    def local_sweeps(design, targets, coef_init, step_sizes, ridge_weights):
        rows, feats = design.shape
        tgt = targets.shape[1]
        half = tgt // CHAINS
        n_fb, n_sb = feats // BIG, rows // BIG
        n_tg = n_feat // (rows // TILE)
        th = half // n_tg
        f32, bf16 = jnp.float32, jnp.bfloat16
        hbm = pl.BlockSpec(memory_space=pl.ANY)
        vmem = pl.BlockSpec(memory_space=pltpu.VMEM)
        w, r = pl.pallas_call(
            functools.partial(_kernel, side, n_feat, n_samp),
            name="descent",
            out_shape=(pltpu.VMEM((feats, tgt), f32), pltpu.VMEM((rows, tgt), f32)),
            in_specs=[hbm, hbm, hbm, vmem, vmem],
            out_specs=(vmem, vmem),
            scratch_shapes=[
                pltpu.VMEM((rows, feats), bf16),
                pltpu.VMEM((feats, rows), bf16),
                pltpu.VMEM((feats, tgt), f32),
                pltpu.VMEM((CHAINS, n_fb, half, BIG), f32),
                pltpu.VMEM((CHAINS, half, feats), bf16),
                pltpu.VMEM((CHAINS, n_feat, th, TILE), bf16),
                pltpu.VMEM((CHAINS, n_feat, th, TILE), bf16),
                pltpu.VMEM((CHAINS, n_feat, th, TILE), bf16),
                pltpu.VMEM((CHAINS, n_fb, half, BIG), f32),
                pltpu.VMEM((2, CHAINS, n_fb, half, BIG), f32),
                pltpu.VMEM((CHAINS, th, TILE), f32),
                pltpu.VMEM((CHAINS, n_feat, th, TILE), f32),
                pltpu.VMEM((TILE, tgt), f32),
                pltpu.VMEM((tgt, tgt), f32),
                pltpu.SemaphoreType.DMA((n_sb,)),
                pltpu.SemaphoreType.DMA((2,)),
                pltpu.SemaphoreType.DMA((CHAINS,)),
                pltpu.SemaphoreType.DMA((CHAINS,)),
                pltpu.SemaphoreType.DMA((CHAINS,)),
                pltpu.SemaphoreType.DMA((CHAINS, side * side)),
                pltpu.SemaphoreType.DMA((CHAINS,)),
                pltpu.SemaphoreType.DMA((CHAINS, n_fb)),
                pltpu.SemaphoreType.DMA((2, CHAINS, n_fb)),
            ],
            compiler_params=pltpu.CompilerParams(collective_id=0, has_side_effects=True, vmem_limit_bytes=56 * 1024 * 1024),
        )(design, targets, coef_init, step_sizes[None, :], ridge_weights[None, :])
        return pl.pallas_call(
            _write,
            name="write",
            out_shape=(jax.ShapeDtypeStruct(w.shape, f32), jax.ShapeDtypeStruct(r.shape, f32)),
            in_specs=[vmem, vmem],
            out_specs=(hbm, hbm),
            scratch_shapes=[pltpu.SemaphoreType.DMA((2,))],
        )(pltpu.with_memory_space_constraint(w, pltpu.VMEM), pltpu.with_memory_space_constraint(r, pltpu.VMEM))

    return jax.shard_map(local_sweeps, mesh=mesh, in_specs=(design_spec, rows_spec, coef_spec, step_spec, ridge_spec), out_specs=(coef_spec, rows_spec), check_vma=False)
```

```python
import functools

import jax
import jax.numpy as jnp
from jax import lax
from jax.experimental import pallas as pl
from jax.experimental.pallas import tpu as pltpu
from jax.sharding import PartitionSpec as P

SWEEPS = 4
STEP_WEIGHT = 0.5
CHAINS = 2
TILE = 128
BIG = 512
MXU = 256
MESH = pl.DeviceIdType.MESH


def _kernel(side, n_feat, n_samp, x_hbm, y_hbm, w0_hbm, eta_ref, lam_ref, w_out, r_out,
            x_v, xt_v, w_nat, w_t, st, u_buf, rs_recv, rb_full, gt, g_recv, rs_res, rf_full, y_tile, lam_t,
            x_sem, in_sem, rs_ssem, rs_rsem, ag_ssem, ag_psem, ag_rsem, g_ssem, g_rsem):
    rows, feats = x_v.shape
    targets = w_nat.shape[1]
    half = targets // CHAINS
    n_sg = rows // TILE
    n_tg = n_feat // n_sg
    th = half // n_tg
    n_fb, n_sb = feats // BIG, rows // BIG

    def hops(*by):
        return sum(min(d, side - d) for d in by)

    steps = range(side)
    plane = sorted([(a, b) for a in steps for b in steps if a or b], key=lambda o: hops(*o))
    far_first = sorted([(a, b, d) for a in steps for b in steps for d in steps if a or b or d],
                       key=lambda o: (-hops(*o), (o[0] + 3 * o[1] + 5 * o[2]) % 7))
    per_sb = n_feat // n_sb
    total_rows = rows * n_samp

    me = lax.axis_index("feat")
    core = lax.axis_index("samp")

    barrier = pltpu.get_barrier_semaphore()

    def greet(d, _):
        pl.semaphore_signal(barrier, inc=1, device_id={"feat": (me + d) % n_feat}, device_id_type=MESH)
        return 0

    lax.fori_loop(1, n_feat, greet, 0)
    pl.semaphore_signal(barrier, inc=1, device_id={"samp": 1 - core}, device_id_type=MESH)

    w_load = pltpu.make_async_copy(w0_hbm, w_nat, in_sem.at[0])
    w_load.start()

    mz, my, mx = me // (side * side), (me // side) % side, me % side
    my_sb, my_in_sb = (mx + my + mz) % side, mz * side + my
    pos = my_sb * per_sb + my_in_sb

    def block_rows(k):
        return pl.ds(pl.multiple_of(((my_sb + k + 1) % n_sb) * BIG, BIG), BIG)

    def x_load(k):
        return pltpu.make_async_copy(x_hbm.at[block_rows(k)], x_v.at[block_rows(k)], x_sem.at[k])

    for k in range(n_sb):
        x_load(k).start()
    my_sg, my_tg = pos // n_tg, pos % n_tg
    y_load = pltpu.make_async_copy(y_hbm.at[pl.ds(pl.multiple_of(my_sg * TILE, TILE), TILE)], y_tile, in_sem.at[1])
    y_load.start()

    def rs_copy(c, place, peer):
        return pltpu.make_async_remote_copy(src_ref=u_buf.at[c, place], dst_ref=rs_recv.at[c, pos], send_sem=rs_ssem.at[c],
                                            recv_sem=rs_rsem.at[c], device_id={"feat": peer}, device_id_type=MESH)

    def rs_all(c):
        return pltpu.make_async_remote_copy(src_ref=u_buf.at[c, pl.ds(1, n_feat - 1)], dst_ref=rs_recv.at[c, pl.ds(1, n_feat - 1)],
                                            send_sem=rs_ssem.at[c], recv_sem=rs_rsem.at[c], device_id={"feat": me},
                                            device_id_type=MESH)

    def keep_tiles(c, k, u):
        sb = (my_sb + k + 1) % n_sb
        for j in range(per_sb):
            g, t = j // n_tg, j % n_tg
            u_buf[c, sb * per_sb + j] = u[t * th:(t + 1) * th, g * TILE:(g + 1) * TILE].astype(jnp.bfloat16)

    def send_tiles(c, k):
        sb = (my_sb + k + 1) % n_sb

        def send(dz, dy, when):
            z, y = (mz + dz) % side, (my + dy) % side
            x = (sb + 2 * side - z - y) % side
            copy = rs_copy(c, sb * per_sb + z * side + y, z * side * side + y * side + x)
            if when is True:
                copy.start()
            else:
                pl.when(when)(copy.start)

        for a, b in reversed(plane):
            send(a, b, True)
        send(0, 0, k != n_sb - 1)

    def reduce(c, coef):
        rs_all(c).wait_recv()
        rs_recv[c, pos] = u_buf[c, pos]
        accs = [rs_recv[c, j].astype(jnp.float32) for j in range(4)]
        for j in range(4, n_feat):
            accs[j % 4] = accs[j % 4] + rs_recv[c, j].astype(jnp.float32)
        total = (accs[0] + accs[1]) + (accs[2] + accs[3])
        rs_res[c] = rs_res[c] - coef * total

    def place_of(device):
        z, y, x = device // (side * side), (device // side) % side, device % side
        return (x + y + z) % side * per_sb + z * side + y

    def axes(first_axis):
        kinds = (first_axis, (first_axis + 1) % 3, (first_axis + 2) % 3)
        strides = [jnp.where(d == 0, 1, jnp.where(d == 1, side, side * side)) for d in kinds]
        return [(stride, (me // stride) % side) for stride in strides]

    def moved(axis, by):
        stride, at = axis
        return ((at + by) % side - at) * stride

    def gather_copy(c, ref, place, peer, recv_sem):
        return pltpu.make_async_remote_copy(src_ref=ref.at[c, place], dst_ref=ref.at[c, place], send_sem=ag_ssem.at[c],
                                            recv_sem=recv_sem, device_id={"feat": peer}, device_id_type=MESH)

    def gather_start(c):
        moves = [[moved(axis, by) for by in range(side)] for axis in axes(core % 3)]
        for a, b, d in far_first:
            gather_copy(c, rb_full, pos, me + moves[0][a] + moves[1][b] + moves[2][d], ag_rsem.at[c]).start()

    def pass_on(c, place):
        ring = axes((c * n_samp + core) % 3)[0]
        for d in range(side - 1, 0, -1):
            gather_copy(c, rf_full, place, me + moved(ring, d), ag_rsem.at[c]).start()

    def last_gather_start(c):
        _, one, two = axes((c * n_samp + core) % 3)
        for i in range(len(plane) - 1, -1, -1):
            a, b = plane[i]
            gather_copy(c, rf_full, pos, me + moved(one, a) + moved(two, b), ag_psem.at[c, i]).start()
        pass_on(c, pos)

    def last_gather_forward(c):
        _, one, two = axes((c * n_samp + core) % 3)
        for i, (a, b) in enumerate(plane):
            place = place_of(me + moved(one, side - a) + moved(two, side - b))
            gather_copy(c, rf_full, place, me, ag_psem.at[c, i]).wait_recv()
            pass_on(c, place)

    def gather_wait(c, ref, tiles):
        part = ref.at[c, pl.ds(0, tiles)]
        pltpu.make_async_remote_copy(src_ref=part, dst_ref=part, send_sem=ag_ssem.at[c], recv_sem=ag_rsem.at[c],
                                     device_id={"feat": me}, device_id_type=MESH).wait_recv()

    def gather_sent(c, ref):
        part = ref.at[c, pl.ds(1, n_feat - 1)]
        pltpu.make_async_remote_copy(src_ref=part, dst_ref=part, send_sem=ag_ssem.at[c], recv_sem=ag_rsem.at[c],
                                     device_id={"feat": me}, device_id_type=MESH).wait_send()

    def g_copy(c, par, f):
        return pltpu.make_async_remote_copy(src_ref=gt.at[c, f], dst_ref=g_recv.at[par, c, f], send_sem=g_ssem.at[c, f],
                                            recv_sem=g_rsem.at[par, c, f], device_id={"samp": 1 - core}, device_id_type=MESH)

    w_load.wait()
    for f in range(n_fb):
        wt = w_nat[f * BIG:(f + 1) * BIG, :].T
        for c in range(CHAINS):
            w_t[c, f] = wt[c * half:(c + 1) * half]
            st[c, :, f * BIG:(f + 1) * BIG] = wt[c * half:(c + 1) * half].astype(jnp.bfloat16)
    lam_t[...] = jnp.broadcast_to(lam_ref[...], (targets, targets)).T

    def first(k, _):
        x_load(k).wait()
        u = lax.dot_general(st[...].reshape(targets, feats), x_v[block_rows(k), :], (((1,), (1,)), ((), ())),
                            preferred_element_type=jnp.float32)
        for c in range(CHAINS):
            keep_tiles(c, k, u[c * half:(c + 1) * half])

        @pl.when(k == 0)
        def _():
            pl.semaphore_wait(barrier, n_feat)
        send_tiles(0, k)
        return 0

    lax.fori_loop(0, n_sb, first, 0)
    lax.fori_loop(0, n_sb, lambda k, _: (send_tiles(1, k), 0)[1], 0)

    eye = (lax.broadcasted_iota(jnp.int32, (MXU, MXU), 0) == lax.broadcasted_iota(jnp.int32, (MXU, MXU), 1)).astype(jnp.bfloat16)

    def turn(r, _):
        piece = pl.ds(pl.multiple_of(r * MXU, MXU), MXU)
        for f in range(0, feats, MXU):
            turned = lax.dot_general(eye, x_v[piece, f:f + MXU], (((1,), (1,)), ((), ())), preferred_element_type=jnp.float32)
            xt_v[f:f + MXU, piece] = turned.astype(jnp.bfloat16)
        return 0

    lax.fori_loop(0, rows // MXU // 2, turn, 0)
    y_load.wait()
    y_tile[...] = y_tile[...].T

    def behind(c, coef, last):
        reduce(c, coef)
        if last:
            rf_full[c, pos] = rs_res[c]
            last_gather_start(c)
        else:
            rb_full[c, pos] = rs_res[c].astype(jnp.bfloat16)
            gather_start(c)
        rs_all(c).wait_send()

    def gradient_part(c, par):
        gather_wait(c, rb_full, n_feat - 1)
        rbt = jnp.concatenate([rb_full[c, g * n_tg:(g + 1) * n_tg].reshape(half, TILE) for g in range(n_sg)], axis=1)

        def grad(f, _):
            cols = pl.ds(pl.multiple_of(f * BIG, BIG), BIG)
            gt[c, f] = jnp.dot(rbt, x_v[:, cols], preferred_element_type=jnp.float32)
            g_copy(c, par, f).start()
            return 0

        lax.fori_loop(0, n_fb, grad, 0)

    def step_and_product(c, par):
        lam = lam_t[c * half:(c + 1) * half, :]
        lam = jnp.concatenate([lam] * (BIG // targets), axis=1)

        def step(f, _):
            g_copy(c, par, f).wait_recv()
            cols = pl.ds(pl.multiple_of(f * BIG, BIG), BIG)
            gradient = (gt[c, f] + g_recv[par, c, f]) / total_rows
            w = w_t[c, f]
            delta = eta_ref[:, cols] * (gradient - lam * w)
            w_t[c, f] = w + STEP_WEIGHT * delta
            st[c, :, cols] = delta.astype(jnp.bfloat16)
            return 0

        lax.fori_loop(0, n_fb, step, 0)
        gather_sent(c, rb_full)

        def product(k, _):
            keep_tiles(c, k, jnp.dot(st[c], xt_v[:, block_rows(k)], preferred_element_type=jnp.float32))
            send_tiles(c, k)
            return 0

        lax.fori_loop(0, n_sb, product, 0)
        for f in range(n_fb):
            g_copy(c, par, f).wait_send()

    def sweep(s, last):
        par = s % 2
        for c in range(CHAINS):
            gradient_part(c, par)
            step_and_product(c, par)
        if last:
            for f in range(n_fb):
                w_out[f * BIG:(f + 1) * BIG, :] = jnp.concatenate([w_t[c, f] for c in range(CHAINS)], axis=0).T
        for c in range(CHAINS):
            behind(c, STEP_WEIGHT, last)

    for c in range(CHAINS):
        rs_res[c] = y_tile[pl.ds(pl.multiple_of(c * half + my_tg * th, th), th), :]
    for c in range(CHAINS):
        behind(c, 1.0, False)
    lax.fori_loop(rows // MXU // 2, rows // MXU, turn, 0)
    lax.fori_loop(0, SWEEPS - 1, lambda s, _: (sweep(s, False), 0)[1], 0)
    sweep(SWEEPS - 1, True)
    for c in range(CHAINS):
        last_gather_forward(c)

    for c in range(CHAINS):
        gather_wait(c, rf_full, n_feat - side * side)
    for g in range(n_sg):
        both = jnp.concatenate([rf_full[c, g * n_tg:(g + 1) * n_tg].reshape(half, TILE) for c in range(CHAINS)], axis=0)
        r_out[g * TILE:(g + 1) * TILE, :] = both.T
    for c in range(CHAINS):
        gather_sent(c, rf_full)


def _write(w_ref, r_ref, w_out, r_out, sem):
    copies = [pltpu.make_async_copy(w_ref, w_out, sem.at[0]), pltpu.make_async_copy(r_ref, r_out, sem.at[1])]
    for copy in copies:
        copy.start()
    for copy in copies:
        copy.wait()


def solution(mesh):
    n_samp, n_feat = mesh.shape["samp"], mesh.shape["feat"]
    side = round(n_feat ** (1 / 3))
    design_spec = P(("problem", "samp"), "feat")
    rows_spec = P(("problem", "samp"), None)
    coef_spec = P(("problem", "feat"), None)
    step_spec = P(("problem", "feat"))
    ridge_spec = P("problem")

    def local_sweeps(design, targets, coef_init, step_sizes, ridge_weights):
        rows, feats = design.shape
        tgt = targets.shape[1]
        half = tgt // CHAINS
        n_fb, n_sb = feats // BIG, rows // BIG
        n_tg = n_feat // (rows // TILE)
        th = half // n_tg
        f32, bf16 = jnp.float32, jnp.bfloat16
        hbm = pl.BlockSpec(memory_space=pl.ANY)
        vmem = pl.BlockSpec(memory_space=pltpu.VMEM)
        w, r = pl.pallas_call(
            functools.partial(_kernel, side, n_feat, n_samp),
            name="descent",
            out_shape=(pltpu.VMEM((feats, tgt), f32), pltpu.VMEM((rows, tgt), f32)),
            in_specs=[hbm, hbm, hbm, vmem, vmem],
            out_specs=(vmem, vmem),
            scratch_shapes=[
                pltpu.VMEM((rows, feats), bf16),
                pltpu.VMEM((feats, rows), bf16),
                pltpu.VMEM((feats, tgt), f32),
                pltpu.VMEM((CHAINS, n_fb, half, BIG), f32),
                pltpu.VMEM((CHAINS, half, feats), bf16),
                pltpu.VMEM((CHAINS, n_feat, th, TILE), bf16),
                pltpu.VMEM((CHAINS, n_feat, th, TILE), bf16),
                pltpu.VMEM((CHAINS, n_feat, th, TILE), bf16),
                pltpu.VMEM((CHAINS, n_fb, half, BIG), f32),
                pltpu.VMEM((2, CHAINS, n_fb, half, BIG), f32),
                pltpu.VMEM((CHAINS, th, TILE), f32),
                pltpu.VMEM((CHAINS, n_feat, th, TILE), f32),
                pltpu.VMEM((TILE, tgt), f32),
                pltpu.VMEM((tgt, tgt), f32),
                pltpu.SemaphoreType.DMA((n_sb,)),
                pltpu.SemaphoreType.DMA((2,)),
                pltpu.SemaphoreType.DMA((CHAINS,)),
                pltpu.SemaphoreType.DMA((CHAINS,)),
                pltpu.SemaphoreType.DMA((CHAINS,)),
                pltpu.SemaphoreType.DMA((CHAINS, side * side)),
                pltpu.SemaphoreType.DMA((CHAINS,)),
                pltpu.SemaphoreType.DMA((CHAINS, n_fb)),
                pltpu.SemaphoreType.DMA((2, CHAINS, n_fb)),
            ],
            compiler_params=pltpu.CompilerParams(collective_id=0, has_side_effects=True, vmem_limit_bytes=56 * 1024 * 1024),
        )(design, targets, coef_init, step_sizes[None, :], ridge_weights[None, :])
        return pl.pallas_call(
            _write,
            name="write",
            out_shape=(jax.ShapeDtypeStruct(w.shape, f32), jax.ShapeDtypeStruct(r.shape, f32)),
            in_specs=[vmem, vmem],
            out_specs=(hbm, hbm),
            scratch_shapes=[pltpu.SemaphoreType.DMA((2,))],
        )(pltpu.with_memory_space_constraint(w, pltpu.VMEM), pltpu.with_memory_space_constraint(r, pltpu.VMEM))

    return jax.shard_map(local_sweeps, mesh=mesh, in_specs=(design_spec, rows_spec, coef_spec, step_spec, ridge_spec), out_specs=(coef_spec, rows_spec), check_vma=False)
```

```python
import functools

import jax
import jax.numpy as jnp
from jax import lax
from jax.experimental import pallas as pl
from jax.experimental.pallas import tpu as pltpu
from jax.sharding import PartitionSpec as P

SWEEPS = 4
STEP_WEIGHT = 0.5
CHAINS = 2
TILE = 128
BIG = 512
MXU = 256
MESH = pl.DeviceIdType.MESH


def _kernel(side, n_feat, n_samp, x_hbm, y_hbm, w0_hbm, eta_ref, lam_ref, w_out, r_out,
            x_v, xt_v, w_nat, w_t, st, u_buf, rs_recv, rb_full, gt, g_recv, rs_res, rf_full, y_tile, lam_t,
            x_sem, in_sem, rs_ssem, rs_rsem, ag_ssem, ag_psem, ag_rsem, g_ssem, g_rsem):
    rows, feats = x_v.shape
    targets = w_nat.shape[1]
    half = targets // CHAINS
    n_sg = rows // TILE
    n_tg = n_feat // n_sg
    th = half // n_tg
    n_fb, n_sb = feats // BIG, rows // BIG

    def hops(*by):
        return sum(min(d, side - d) for d in by)

    steps = range(side)
    plane = sorted([(a, b) for a in steps for b in steps if a or b], key=lambda o: hops(*o))
    far_first = sorted([(a, b, d) for a in steps for b in steps for d in steps if a or b or d],
                       key=lambda o: (-hops(*o), (o[0] + 3 * o[1] + 5 * o[2]) % 7))
    arrive = sorted(steps, key=lambda q: max(hops(*o) for o in far_first if sum(o) % side == q))
    per_sb = n_feat // n_sb
    total_rows = rows * n_samp

    me = lax.axis_index("feat")
    core = lax.axis_index("samp")

    barrier = pltpu.get_barrier_semaphore()

    def greet(d, _):
        pl.semaphore_signal(barrier, inc=1, device_id={"feat": (me + d) % n_feat}, device_id_type=MESH)
        return 0

    lax.fori_loop(1, n_feat, greet, 0)
    pl.semaphore_signal(barrier, inc=1, device_id={"samp": 1 - core}, device_id_type=MESH)

    w_load = pltpu.make_async_copy(w0_hbm, w_nat, in_sem.at[0])
    w_load.start()

    mz, my, mx = me // (side * side), (me // side) % side, me % side
    my_sb, my_in_sb = (mx + my + mz) % side, mz * side + my
    pos = my_sb * per_sb + my_in_sb

    def class_of(k):
        return sum(jnp.where(k == i, q, 0) for i, q in enumerate(reversed(arrive)))

    def block_of(k):
        return (my_sb + class_of(k)) % n_sb

    def block_rows(k):
        return pl.ds(pl.multiple_of(block_of(k) * BIG, BIG), BIG)

    def x_load(k):
        return pltpu.make_async_copy(x_hbm.at[block_rows(k)], x_v.at[block_rows(k)], x_sem.at[k])

    x_load(0).start()
    my_sg, my_tg = pos // n_tg, pos % n_tg
    y_load = pltpu.make_async_copy(y_hbm.at[pl.ds(pl.multiple_of(my_sg * TILE, TILE), TILE)], y_tile, in_sem.at[1])

    def rs_copy(c, place, peer):
        return pltpu.make_async_remote_copy(src_ref=u_buf.at[c, place], dst_ref=rs_recv.at[c, pos], send_sem=rs_ssem.at[c],
                                            recv_sem=rs_rsem.at[c], device_id={"feat": peer}, device_id_type=MESH)

    def rs_all(c):
        return pltpu.make_async_remote_copy(src_ref=u_buf.at[c, pl.ds(1, n_feat - 1)], dst_ref=rs_recv.at[c, pl.ds(1, n_feat - 1)],
                                            send_sem=rs_ssem.at[c], recv_sem=rs_rsem.at[c], device_id={"feat": me},
                                            device_id_type=MESH)

    def keep_tiles(c, k, u):
        sb = block_of(k)
        for j in range(per_sb):
            g, t = j // n_tg, j % n_tg
            u_buf[c, sb * per_sb + j] = u[t * th:(t + 1) * th, g * TILE:(g + 1) * TILE].astype(jnp.bfloat16)

    def send_tiles(c, k):
        sb = block_of(k)

        def send(dz, dy, when):
            z, y = (mz + dz) % side, (my + dy) % side
            x = (sb + 2 * side - z - y) % side
            copy = rs_copy(c, sb * per_sb + z * side + y, z * side * side + y * side + x)
            if when is True:
                copy.start()
            else:
                pl.when(when)(copy.start)

        for a, b in reversed(plane):
            send(a, b, True)
        send(0, 0, k != n_sb - 1)

    def reduce(c, coef):
        rs_all(c).wait_recv()
        rs_recv[c, pos] = u_buf[c, pos]
        accs = [rs_recv[c, j].astype(jnp.float32) for j in range(4)]
        for j in range(4, n_feat):
            accs[j % 4] = accs[j % 4] + rs_recv[c, j].astype(jnp.float32)
        total = (accs[0] + accs[1]) + (accs[2] + accs[3])
        rs_res[c] = rs_res[c] - coef * total

    def place_of(device):
        z, y, x = device // (side * side), (device // side) % side, device % side
        return (x + y + z) % side * per_sb + z * side + y

    def axes(first_axis):
        kinds = (first_axis, (first_axis + 1) % 3, (first_axis + 2) % 3)
        strides = [jnp.where(d == 0, 1, jnp.where(d == 1, side, side * side)) for d in kinds]
        return [(stride, (me // stride) % side) for stride in strides]

    def moved(axis, by):
        stride, at = axis
        return ((at + by) % side - at) * stride

    def gather_copy(c, ref, place, peer, recv_sem):
        return pltpu.make_async_remote_copy(src_ref=ref.at[c, place], dst_ref=ref.at[c, place], send_sem=ag_ssem.at[c],
                                            recv_sem=recv_sem, device_id={"feat": peer}, device_id_type=MESH)

    def gather_start(c):
        moves = [[moved(axis, by) for by in range(side)] for axis in axes(core % 3)]
        for a, b, d in far_first:
            gather_copy(c, rb_full, pos, me + moves[0][a] + moves[1][b] + moves[2][d],
                        ag_rsem.at[c, (a + b + d) % side]).start()

    def pass_on(c, place):
        ring = axes((c * n_samp + core) % 3)[0]
        for d in range(side - 1, 0, -1):
            gather_copy(c, rf_full, place, me + moved(ring, d), ag_rsem.at[c, 0]).start()

    def last_gather_start(c):
        _, one, two = axes((c * n_samp + core) % 3)
        for i in range(len(plane) - 1, -1, -1):
            a, b = plane[i]
            gather_copy(c, rf_full, pos, me + moved(one, a) + moved(two, b), ag_psem.at[c, i]).start()
        pass_on(c, pos)

    def last_gather_forward(c):
        _, one, two = axes((c * n_samp + core) % 3)
        for i, (a, b) in enumerate(plane):
            place = place_of(me + moved(one, side - a) + moved(two, side - b))
            gather_copy(c, rf_full, place, me, ag_psem.at[c, i]).wait_recv()
            pass_on(c, place)

    def gather_wait(c, ref, tiles, q):
        part = ref.at[c, pl.ds(0, tiles)]
        pltpu.make_async_remote_copy(src_ref=part, dst_ref=part, send_sem=ag_ssem.at[c], recv_sem=ag_rsem.at[c, q],
                                     device_id={"feat": me}, device_id_type=MESH).wait_recv()

    def gather_sent(c, ref):
        part = ref.at[c, pl.ds(1, n_feat - 1)]
        pltpu.make_async_remote_copy(src_ref=part, dst_ref=part, send_sem=ag_ssem.at[c], recv_sem=ag_rsem.at[c, 0],
                                     device_id={"feat": me}, device_id_type=MESH).wait_send()

    def g_copy(c, par, f):
        return pltpu.make_async_remote_copy(src_ref=gt.at[c, f], dst_ref=g_recv.at[par, c, f], send_sem=g_ssem.at[c, f],
                                            recv_sem=g_rsem.at[par, c, f], device_id={"samp": 1 - core}, device_id_type=MESH)

    w_load.wait()
    for k in range(1, n_sb):
        x_load(k).start()
    y_load.start()
    for f in range(n_fb):
        wt = w_nat[f * BIG:(f + 1) * BIG, :].T
        for c in range(CHAINS):
            w_t[c, f] = wt[c * half:(c + 1) * half]
            st[c, :, f * BIG:(f + 1) * BIG] = wt[c * half:(c + 1) * half].astype(jnp.bfloat16)
    lam_t[...] = jnp.broadcast_to(lam_ref[...], (targets, targets)).T

    def first(k, _):
        x_load(k).wait()
        u = lax.dot_general(st[...].reshape(targets, feats), x_v[block_rows(k), :], (((1,), (1,)), ((), ())),
                            preferred_element_type=jnp.float32)
        for c in range(CHAINS):
            keep_tiles(c, k, u[c * half:(c + 1) * half])

        @pl.when(k == 0)
        def _():
            pl.semaphore_wait(barrier, n_feat)
        send_tiles(0, k)
        return 0

    lax.fori_loop(0, n_sb, first, 0)
    lax.fori_loop(0, n_sb, lambda k, _: (send_tiles(1, k), 0)[1], 0)

    eye = (lax.broadcasted_iota(jnp.int32, (MXU, MXU), 0) == lax.broadcasted_iota(jnp.int32, (MXU, MXU), 1)).astype(jnp.bfloat16)

    def turn(r, _):
        piece = pl.ds(pl.multiple_of(r * MXU, MXU), MXU)
        for f in range(0, feats, MXU):
            turned = lax.dot_general(eye, x_v[piece, f:f + MXU], (((1,), (1,)), ((), ())), preferred_element_type=jnp.float32)
            xt_v[f:f + MXU, piece] = turned.astype(jnp.bfloat16)
        return 0

    lax.fori_loop(0, rows // MXU // 2, turn, 0)
    y_load.wait()
    y_tile[...] = y_tile[...].T

    def behind(c, coef, last):
        reduce(c, coef)
        if last:
            rf_full[c, pos] = rs_res[c]
            last_gather_start(c)
        else:
            rb_full[c, pos] = rs_res[c].astype(jnp.bfloat16)
            gather_start(c)
        rs_all(c).wait_send()

    def gradient_part(c, par):
        for n, q in enumerate(arrive):
            gather_wait(c, rb_full, per_sb - (q == 0), q)
            sb = (my_sb + side - q) % n_sb
            block = pl.ds(pl.multiple_of(sb * BIG, BIG), BIG)
            rbt = jnp.concatenate([rb_full[c, pl.ds(sb * per_sb + g * n_tg, n_tg)].reshape(half, TILE) for g in range(BIG // TILE)], axis=1)
            for f in range(n_fb):
                part = jnp.dot(rbt, x_v[block, f * BIG:(f + 1) * BIG], preferred_element_type=jnp.float32)
                gt[c, f] = part if n == 0 else gt[c, f] + part
                if n == len(arrive) - 1:
                    g_copy(c, par, f).start()

    def step_and_product(c, par):
        lam = lam_t[c * half:(c + 1) * half, :]
        lam = jnp.concatenate([lam] * (BIG // targets), axis=1)

        def step(f, _):
            g_copy(c, par, f).wait_recv()
            cols = pl.ds(pl.multiple_of(f * BIG, BIG), BIG)
            gradient = (gt[c, f] + g_recv[par, c, f]) / total_rows
            w = w_t[c, f]
            delta = eta_ref[:, cols] * (gradient - lam * w)
            w_t[c, f] = w + STEP_WEIGHT * delta
            st[c, :, cols] = delta.astype(jnp.bfloat16)
            return 0

        lax.fori_loop(0, n_fb, step, 0)
        gather_sent(c, rb_full)

        def product(k, _):
            keep_tiles(c, k, jnp.dot(st[c], xt_v[:, block_rows(k)], preferred_element_type=jnp.float32))
            send_tiles(c, k)
            return 0

        lax.fori_loop(0, n_sb, product, 0)
        for f in range(n_fb):
            g_copy(c, par, f).wait_send()

    def sweep(s, last):
        par = s % 2
        for c in range(CHAINS):
            gradient_part(c, par)
            step_and_product(c, par)
        if last:
            for f in range(n_fb):
                w_out[f * BIG:(f + 1) * BIG, :] = jnp.concatenate([w_t[c, f] for c in range(CHAINS)], axis=0).T
        for c in range(CHAINS):
            behind(c, STEP_WEIGHT, last)

    for c in range(CHAINS):
        rs_res[c] = y_tile[pl.ds(pl.multiple_of(c * half + my_tg * th, th), th), :]
    for c in range(CHAINS):
        behind(c, 1.0, False)
    lax.fori_loop(rows // MXU // 2, rows // MXU, turn, 0)
    lax.fori_loop(0, SWEEPS - 1, lambda s, _: (sweep(s, False), 0)[1], 0)
    sweep(SWEEPS - 1, True)
    for c in range(CHAINS):
        last_gather_forward(c)

    for c in range(CHAINS):
        gather_wait(c, rf_full, n_feat - side * side, 0)
    for g in range(n_sg):
        both = jnp.concatenate([rf_full[c, g * n_tg:(g + 1) * n_tg].reshape(half, TILE) for c in range(CHAINS)], axis=0)
        r_out[g * TILE:(g + 1) * TILE, :] = both.T
    for c in range(CHAINS):
        gather_sent(c, rf_full)


def _write(w_ref, r_ref, w_out, r_out, sem):
    copies = [pltpu.make_async_copy(w_ref, w_out, sem.at[0]), pltpu.make_async_copy(r_ref, r_out, sem.at[1])]
    for copy in copies:
        copy.start()
    for copy in copies:
        copy.wait()


def solution(mesh):
    n_samp, n_feat = mesh.shape["samp"], mesh.shape["feat"]
    side = round(n_feat ** (1 / 3))
    design_spec = P(("problem", "samp"), "feat")
    rows_spec = P(("problem", "samp"), None)
    coef_spec = P(("problem", "feat"), None)
    step_spec = P(("problem", "feat"))
    ridge_spec = P("problem")

    def local_sweeps(design, targets, coef_init, step_sizes, ridge_weights):
        rows, feats = design.shape
        tgt = targets.shape[1]
        half = tgt // CHAINS
        n_fb, n_sb = feats // BIG, rows // BIG
        n_tg = n_feat // (rows // TILE)
        th = half // n_tg
        f32, bf16 = jnp.float32, jnp.bfloat16
        hbm = pl.BlockSpec(memory_space=pl.ANY)
        vmem = pl.BlockSpec(memory_space=pltpu.VMEM)
        w, r = pl.pallas_call(
            functools.partial(_kernel, side, n_feat, n_samp),
            name="descent",
            out_shape=(pltpu.VMEM((feats, tgt), f32), pltpu.VMEM((rows, tgt), f32)),
            in_specs=[hbm, hbm, hbm, vmem, vmem],
            out_specs=(vmem, vmem),
            scratch_shapes=[
                pltpu.VMEM((rows, feats), bf16),
                pltpu.VMEM((feats, rows), bf16),
                pltpu.VMEM((feats, tgt), f32),
                pltpu.VMEM((CHAINS, n_fb, half, BIG), f32),
                pltpu.VMEM((CHAINS, half, feats), bf16),
                pltpu.VMEM((CHAINS, n_feat, th, TILE), bf16),
                pltpu.VMEM((CHAINS, n_feat, th, TILE), bf16),
                pltpu.VMEM((CHAINS, n_feat, th, TILE), bf16),
                pltpu.VMEM((CHAINS, n_fb, half, BIG), f32),
                pltpu.VMEM((2, CHAINS, n_fb, half, BIG), f32),
                pltpu.VMEM((CHAINS, th, TILE), f32),
                pltpu.VMEM((CHAINS, n_feat, th, TILE), f32),
                pltpu.VMEM((TILE, tgt), f32),
                pltpu.VMEM((tgt, tgt), f32),
                pltpu.SemaphoreType.DMA((n_sb,)),
                pltpu.SemaphoreType.DMA((2,)),
                pltpu.SemaphoreType.DMA((CHAINS,)),
                pltpu.SemaphoreType.DMA((CHAINS,)),
                pltpu.SemaphoreType.DMA((CHAINS,)),
                pltpu.SemaphoreType.DMA((CHAINS, side * side)),
                pltpu.SemaphoreType.DMA((CHAINS, side)),
                pltpu.SemaphoreType.DMA((CHAINS, n_fb)),
                pltpu.SemaphoreType.DMA((2, CHAINS, n_fb)),
            ],
            compiler_params=pltpu.CompilerParams(collective_id=0, has_side_effects=True, vmem_limit_bytes=56 * 1024 * 1024),
        )(design, targets, coef_init, step_sizes[None, :], ridge_weights[None, :])
        return pl.pallas_call(
            _write,
            name="write",
            out_shape=(jax.ShapeDtypeStruct(w.shape, f32), jax.ShapeDtypeStruct(r.shape, f32)),
            in_specs=[vmem, vmem],
            out_specs=(hbm, hbm),
            scratch_shapes=[pltpu.SemaphoreType.DMA((2,))],
        )(pltpu.with_memory_space_constraint(w, pltpu.VMEM), pltpu.with_memory_space_constraint(r, pltpu.VMEM))

    return jax.shard_map(local_sweeps, mesh=mesh, in_specs=(design_spec, rows_spec, coef_spec, step_spec, ridge_spec), out_specs=(coef_spec, rows_spec), check_vma=False)
```

```python
import functools

import jax
import jax.numpy as jnp
from jax import lax
from jax.experimental import pallas as pl
from jax.experimental.pallas import tpu as pltpu
from jax.sharding import PartitionSpec as P

SWEEPS = 4
STEP_WEIGHT = 0.5
CHAINS = 2
TILE = 128
BIG = 512
MXU = 256
MESH = pl.DeviceIdType.MESH


def _kernel(side, n_feat, n_samp, x_hbm, y_hbm, w0_hbm, eta_ref, lam_ref, w_out, r_out,
            x_v, xt_v, w_nat, w_t, st, u_buf, rs_recv, rb_full, gt, g_recv, rs_res, rf_full, y_tile, lam_t,
            x_sem, in_sem, rs_ssem, rs_rsem, ag_ssem, ag_psem, ag_rsem, g_ssem, g_rsem):
    rows, feats = x_v.shape
    targets = w_nat.shape[1]
    half = targets // CHAINS
    n_sg = rows // TILE
    n_tg = n_feat // n_sg
    th = half // n_tg
    n_fb, n_sb = feats // BIG, rows // BIG

    def hops(*by):
        return sum(min(d, side - d) for d in by)

    steps = range(side)
    plane = sorted([(a, b) for a in steps for b in steps if a or b], key=lambda o: hops(*o))
    far_first = sorted([(a, b, d) for a in steps for b in steps for d in steps if a or b or d],
                       key=lambda o: (-hops(*o), (o[0] + 3 * o[1] + 5 * o[2]) % 7))
    arrive = sorted(steps, key=lambda q: max(hops(*o) for o in far_first if sum(o) % side == q))
    n_pair = 2 if side > 2 else 1
    per_sb = n_feat // n_sb
    total_rows = rows * n_samp

    me = lax.axis_index("feat")
    core = lax.axis_index("samp")

    barrier = pltpu.get_barrier_semaphore()

    def greet(d, _):
        pl.semaphore_signal(barrier, inc=1, device_id={"feat": (me + d) % n_feat}, device_id_type=MESH)
        return 0

    lax.fori_loop(1, n_feat, greet, 0)
    pl.semaphore_signal(barrier, inc=1, device_id={"samp": 1 - core}, device_id_type=MESH)

    w_load = pltpu.make_async_copy(w0_hbm, w_nat, in_sem.at[0])
    w_load.start()

    mz, my, mx = me // (side * side), (me // side) % side, me % side
    my_sb, my_in_sb = (mx + my + mz) % side, mz * side + my
    pos = my_sb * per_sb + my_in_sb

    def class_of(k):
        return sum(jnp.where(k == i, q, 0) for i, q in enumerate(reversed(arrive)))

    def block_of(k):
        return (my_sb + class_of(k)) % n_sb

    def block_rows(k):
        return pl.ds(pl.multiple_of(block_of(k) * BIG, BIG), BIG)

    def x_load(k):
        return pltpu.make_async_copy(x_hbm.at[block_rows(k)], x_v.at[block_rows(k)], x_sem.at[k])

    x_load(0).start()
    my_sg, my_tg = pos // n_tg, pos % n_tg
    y_load = pltpu.make_async_copy(y_hbm.at[pl.ds(pl.multiple_of(my_sg * TILE, TILE), TILE)], y_tile, in_sem.at[1])

    def rs_copy(c, place, peer):
        return pltpu.make_async_remote_copy(src_ref=u_buf.at[c, place], dst_ref=rs_recv.at[c, pos], send_sem=rs_ssem.at[c],
                                            recv_sem=rs_rsem.at[c], device_id={"feat": peer}, device_id_type=MESH)

    def rs_all(c):
        return pltpu.make_async_remote_copy(src_ref=u_buf.at[c, pl.ds(1, n_feat - 1)], dst_ref=rs_recv.at[c, pl.ds(1, n_feat - 1)],
                                            send_sem=rs_ssem.at[c], recv_sem=rs_rsem.at[c], device_id={"feat": me},
                                            device_id_type=MESH)

    def keep_tiles(c, k, u):
        sb = block_of(k)
        for j in range(per_sb):
            g, t = j // n_tg, j % n_tg
            u_buf[c, sb * per_sb + j] = u[t * th:(t + 1) * th, g * TILE:(g + 1) * TILE].astype(jnp.bfloat16)

    def send_tiles(c, k):
        sb = block_of(k)

        def send(dz, dy, when):
            z, y = (mz + dz) % side, (my + dy) % side
            x = (sb + 2 * side - z - y) % side
            copy = rs_copy(c, sb * per_sb + z * side + y, z * side * side + y * side + x)
            if when is True:
                copy.start()
            else:
                pl.when(when)(copy.start)

        for a, b in reversed(plane):
            send(a, b, True)
        send(0, 0, k != n_sb - 1)

    def reduce(c, coef):
        rs_all(c).wait_recv()
        rs_recv[c, pos] = u_buf[c, pos]
        accs = [rs_recv[c, j].astype(jnp.float32) for j in range(4)]
        for j in range(4, n_feat):
            accs[j % 4] = accs[j % 4] + rs_recv[c, j].astype(jnp.float32)
        total = (accs[0] + accs[1]) + (accs[2] + accs[3])
        rs_res[c] = rs_res[c] - coef * total

    def place_of(device):
        z, y, x = device // (side * side), (device // side) % side, device % side
        return (x + y + z) % side * per_sb + z * side + y

    def axes(first_axis):
        kinds = (first_axis, (first_axis + 1) % 3, (first_axis + 2) % 3)
        strides = [jnp.where(d == 0, 1, jnp.where(d == 1, side, side * side)) for d in kinds]
        return [(stride, (me // stride) % side) for stride in strides]

    def moved(axis, by):
        stride, at = axis
        return ((at + by) % side - at) * stride

    def gather_copy(c, ref, place, peer, recv_sem):
        return pltpu.make_async_remote_copy(src_ref=ref.at[c, place], dst_ref=ref.at[c, place], send_sem=ag_ssem.at[c],
                                            recv_sem=recv_sem, device_id={"feat": peer}, device_id_type=MESH)

    def first_stop(i):
        def near(n):
            return n + jnp.where(n == 2, 1, 0) - jnp.where(n == 3, 1, 0)

        return lax.rem(i, n_pair) * (side - 1), near(lax.rem(lax.div(i, n_pair), side)), near(lax.div(i, n_pair * side))

    def hop_on(c, place, i):
        third = axes((c * n_samp + core) % 3)[0]
        peer = me + jnp.where(lax.rem(i, n_pair) == 0, moved(third, 1), moved(third, side - 1))
        gather_copy(c, rb_full, place, peer, ag_rsem.at[c]).start()

    def gather_start(c):
        (st0, at0), (st1, at1), (st2, at2) = axes((c * n_samp + core) % 3)

        def send(n, _):
            i = n_pair * side * side - 1 - n
            r, a, b = first_stop(i)
            peer = lax.rem(at0 + r, side) * st0 + lax.rem(at1 + a, side) * st1 + lax.rem(at2 + b, side) * st2
            gather_copy(c, rb_full, pos, peer, ag_psem.at[c, i]).start()
            return 0

        lax.fori_loop(0, n_pair * side * side - 1, send, 0)
        hop_on(c, pos, 0)

    def gather_forward(c):
        (st0, at0), (st1, at1), (st2, at2) = axes((c * n_samp + core) % 3)

        def forward(i, _):
            r, a, b = first_stop(i)
            t, u, v = lax.rem(at0 + side - r, side), lax.rem(at1 + side - a, side), lax.rem(at2 + side - b, side)
            place = lax.rem(t + u + v, side) * per_sb + lax.div(t * st0 + u * st1 + v * st2, side)
            gather_copy(c, rb_full, place, me, ag_psem.at[c, i]).wait_recv()
            hop_on(c, place, i)
            return 0

        lax.fori_loop(1, n_pair * side * side, forward, 0)

    def pass_on(c, place):
        ring = axes((c * n_samp + core) % 3)[0]
        for d in range(side - 1, 0, -1):
            gather_copy(c, rf_full, place, me + moved(ring, d), ag_rsem.at[c]).start()

    def last_gather_start(c):
        _, one, two = axes((c * n_samp + core) % 3)
        for i in range(len(plane) - 1, -1, -1):
            a, b = plane[i]
            gather_copy(c, rf_full, pos, me + moved(one, a) + moved(two, b), ag_psem.at[c, i]).start()
        pass_on(c, pos)

    def last_gather_forward(c):
        _, one, two = axes((c * n_samp + core) % 3)
        for i, (a, b) in enumerate(plane):
            place = place_of(me + moved(one, side - a) + moved(two, side - b))
            gather_copy(c, rf_full, place, me, ag_psem.at[c, i]).wait_recv()
            pass_on(c, place)

    def gather_wait(c, ref, tiles):
        part = ref.at[c, pl.ds(0, tiles)]
        pltpu.make_async_remote_copy(src_ref=part, dst_ref=part, send_sem=ag_ssem.at[c], recv_sem=ag_rsem.at[c],
                                     device_id={"feat": me}, device_id_type=MESH).wait_recv()

    def gather_sent(c, ref):
        part = ref.at[c, pl.ds(1, n_feat - 1)]
        pltpu.make_async_remote_copy(src_ref=part, dst_ref=part, send_sem=ag_ssem.at[c], recv_sem=ag_rsem.at[c],
                                     device_id={"feat": me}, device_id_type=MESH).wait_send()

    def g_copy(c, par, f):
        return pltpu.make_async_remote_copy(src_ref=gt.at[c, f], dst_ref=g_recv.at[par, c, f], send_sem=g_ssem.at[c, f],
                                            recv_sem=g_rsem.at[par, c, f], device_id={"samp": 1 - core}, device_id_type=MESH)

    w_load.wait()
    for k in range(1, n_sb):
        x_load(k).start()
    y_load.start()
    for f in range(n_fb):
        wt = w_nat[f * BIG:(f + 1) * BIG, :].T
        for c in range(CHAINS):
            w_t[c, f] = wt[c * half:(c + 1) * half]
            st[c, :, f * BIG:(f + 1) * BIG] = wt[c * half:(c + 1) * half].astype(jnp.bfloat16)
    lam_t[...] = jnp.broadcast_to(lam_ref[...], (targets, targets)).T

    def first(k, _):
        x_load(k).wait()
        u = lax.dot_general(st[...].reshape(targets, feats), x_v[block_rows(k), :], (((1,), (1,)), ((), ())),
                            preferred_element_type=jnp.float32)
        for c in range(CHAINS):
            keep_tiles(c, k, u[c * half:(c + 1) * half])

        @pl.when(k == 0)
        def _():
            pl.semaphore_wait(barrier, n_feat)
        send_tiles(0, k)
        return 0

    lax.fori_loop(0, n_sb, first, 0)
    lax.fori_loop(0, n_sb, lambda k, _: (send_tiles(1, k), 0)[1], 0)

    eye = (lax.broadcasted_iota(jnp.int32, (MXU, MXU), 0) == lax.broadcasted_iota(jnp.int32, (MXU, MXU), 1)).astype(jnp.bfloat16)

    def turn(r, _):
        piece = pl.ds(pl.multiple_of(r * MXU, MXU), MXU)
        for f in range(0, feats, MXU):
            turned = lax.dot_general(eye, x_v[piece, f:f + MXU], (((1,), (1,)), ((), ())), preferred_element_type=jnp.float32)
            xt_v[f:f + MXU, piece] = turned.astype(jnp.bfloat16)
        return 0

    lax.fori_loop(0, rows // MXU // 2, turn, 0)
    y_load.wait()
    y_tile[...] = y_tile[...].T

    def behind(c, coef, last):
        reduce(c, coef)
        if last:
            rf_full[c, pos] = rs_res[c]
            last_gather_start(c)
        else:
            rb_full[c, pos] = rs_res[c].astype(jnp.bfloat16)
            gather_start(c)
        rs_all(c).wait_send()

    def gradient_part(c, par):
        gather_wait(c, rb_full, n_pair * side * side)
        rbt = jnp.concatenate([rb_full[c, g * n_tg:(g + 1) * n_tg].reshape(half, TILE) for g in range(n_sg)], axis=1)

        def grad(f, _):
            cols = pl.ds(pl.multiple_of(f * BIG, BIG), BIG)
            gt[c, f] = jnp.dot(rbt, x_v[:, cols], preferred_element_type=jnp.float32)
            g_copy(c, par, f).start()
            return 0

        lax.fori_loop(0, n_fb, grad, 0)

    def step_and_product(c, par):
        lam = lam_t[c * half:(c + 1) * half, :]
        lam = jnp.concatenate([lam] * (BIG // targets), axis=1)

        def step(f, _):
            g_copy(c, par, f).wait_recv()
            cols = pl.ds(pl.multiple_of(f * BIG, BIG), BIG)
            gradient = (gt[c, f] + g_recv[par, c, f]) / total_rows
            w = w_t[c, f]
            delta = eta_ref[:, cols] * (gradient - lam * w)
            w_t[c, f] = w + STEP_WEIGHT * delta
            st[c, :, cols] = delta.astype(jnp.bfloat16)
            return 0

        lax.fori_loop(0, n_fb, step, 0)
        gather_sent(c, rb_full)

        def product(k, _):
            keep_tiles(c, k, jnp.dot(st[c], xt_v[:, block_rows(k)], preferred_element_type=jnp.float32))
            send_tiles(c, k)
            return 0

        lax.fori_loop(0, n_sb, product, 0)
        for f in range(n_fb):
            g_copy(c, par, f).wait_send()

    def sweep(s, last):
        par = s % 2
        gradient_part(0, par)
        gather_forward(1)
        step_and_product(0, par)
        gradient_part(1, par)
        step_and_product(1, par)
        if last:
            for f in range(n_fb):
                w_out[f * BIG:(f + 1) * BIG, :] = jnp.concatenate([w_t[c, f] for c in range(CHAINS)], axis=0).T
        for c in range(CHAINS):
            behind(c, STEP_WEIGHT, last)
        if not last:
            gather_forward(0)

    for c in range(CHAINS):
        rs_res[c] = y_tile[pl.ds(pl.multiple_of(c * half + my_tg * th, th), th), :]
    for c in range(CHAINS):
        behind(c, 1.0, False)
    lax.fori_loop(rows // MXU // 2, rows // MXU, turn, 0)
    gather_forward(0)
    lax.fori_loop(0, SWEEPS - 1, lambda s, _: (sweep(s, False), 0)[1], 0)
    sweep(SWEEPS - 1, True)
    for c in range(CHAINS):
        last_gather_forward(c)

    for c in range(CHAINS):
        gather_wait(c, rf_full, n_feat - side * side)
    for g in range(n_sg):
        both = jnp.concatenate([rf_full[c, g * n_tg:(g + 1) * n_tg].reshape(half, TILE) for c in range(CHAINS)], axis=0)
        r_out[g * TILE:(g + 1) * TILE, :] = both.T
    for c in range(CHAINS):
        gather_sent(c, rf_full)


def _write(w_ref, r_ref, w_out, r_out, sem):
    copies = [pltpu.make_async_copy(w_ref, w_out, sem.at[0]), pltpu.make_async_copy(r_ref, r_out, sem.at[1])]
    for copy in copies:
        copy.start()
    for copy in copies:
        copy.wait()


def solution(mesh):
    n_samp, n_feat = mesh.shape["samp"], mesh.shape["feat"]
    side = round(n_feat ** (1 / 3))
    design_spec = P(("problem", "samp"), "feat")
    rows_spec = P(("problem", "samp"), None)
    coef_spec = P(("problem", "feat"), None)
    step_spec = P(("problem", "feat"))
    ridge_spec = P("problem")

    def local_sweeps(design, targets, coef_init, step_sizes, ridge_weights):
        rows, feats = design.shape
        tgt = targets.shape[1]
        half = tgt // CHAINS
        n_fb, n_sb = feats // BIG, rows // BIG
        n_tg = n_feat // (rows // TILE)
        th = half // n_tg
        f32, bf16 = jnp.float32, jnp.bfloat16
        hbm = pl.BlockSpec(memory_space=pl.ANY)
        vmem = pl.BlockSpec(memory_space=pltpu.VMEM)
        w, r = pl.pallas_call(
            functools.partial(_kernel, side, n_feat, n_samp),
            name="descent",
            out_shape=(pltpu.VMEM((feats, tgt), f32), pltpu.VMEM((rows, tgt), f32)),
            in_specs=[hbm, hbm, hbm, vmem, vmem],
            out_specs=(vmem, vmem),
            scratch_shapes=[
                pltpu.VMEM((rows, feats), bf16),
                pltpu.VMEM((feats, rows), bf16),
                pltpu.VMEM((feats, tgt), f32),
                pltpu.VMEM((CHAINS, n_fb, half, BIG), f32),
                pltpu.VMEM((CHAINS, half, feats), bf16),
                pltpu.VMEM((CHAINS, n_feat, th, TILE), bf16),
                pltpu.VMEM((CHAINS, n_feat, th, TILE), bf16),
                pltpu.VMEM((CHAINS, n_feat, th, TILE), bf16),
                pltpu.VMEM((CHAINS, n_fb, half, BIG), f32),
                pltpu.VMEM((2, CHAINS, n_fb, half, BIG), f32),
                pltpu.VMEM((CHAINS, th, TILE), f32),
                pltpu.VMEM((CHAINS, n_feat, th, TILE), f32),
                pltpu.VMEM((TILE, tgt), f32),
                pltpu.VMEM((tgt, tgt), f32),
                pltpu.SemaphoreType.DMA((n_sb,)),
                pltpu.SemaphoreType.DMA((2,)),
                pltpu.SemaphoreType.DMA((CHAINS,)),
                pltpu.SemaphoreType.DMA((CHAINS,)),
                pltpu.SemaphoreType.DMA((CHAINS,)),
                pltpu.SemaphoreType.DMA((CHAINS, 2 * side * side)),
                pltpu.SemaphoreType.DMA((CHAINS,)),
                pltpu.SemaphoreType.DMA((CHAINS, n_fb)),
                pltpu.SemaphoreType.DMA((2, CHAINS, n_fb)),
            ],
            compiler_params=pltpu.CompilerParams(collective_id=0, has_side_effects=True, vmem_limit_bytes=56 * 1024 * 1024),
        )(design, targets, coef_init, step_sizes[None, :], ridge_weights[None, :])
        return pl.pallas_call(
            _write,
            name="write",
            out_shape=(jax.ShapeDtypeStruct(w.shape, f32), jax.ShapeDtypeStruct(r.shape, f32)),
            in_specs=[vmem, vmem],
            out_specs=(hbm, hbm),
            scratch_shapes=[pltpu.SemaphoreType.DMA((2,))],
        )(pltpu.with_memory_space_constraint(w, pltpu.VMEM), pltpu.with_memory_space_constraint(r, pltpu.VMEM))

    return jax.shard_map(local_sweeps, mesh=mesh, in_specs=(design_spec, rows_spec, coef_spec, step_spec, ridge_spec), out_specs=(coef_spec, rows_spec), check_vma=False)
```

```python
import functools

import jax
import jax.numpy as jnp
from jax import lax
from jax.experimental import pallas as pl
from jax.experimental.pallas import tpu as pltpu
from jax.sharding import PartitionSpec as P

SWEEPS = 4
STEP_WEIGHT = 0.5
CHAINS = 2
TILE = 128
BIG = 512
MXU = 256
MESH = pl.DeviceIdType.MESH


def _kernel(side, n_feat, n_samp, x_hbm, y_hbm, w0_hbm, eta_ref, lam_ref, w_out, r_out,
            x_v, xt_v, w_nat, w_t, st, u_buf, rs_recv, rb_full, gt, g_recv, rs_res, rf_full, y_tile, lam_t,
            x_sem, in_sem, rs_ssem, rs_rsem, ag_ssem, ag_psem, ag_rsem, g_ssem, g_rsem):
    rows, feats = x_v.shape
    targets = w_nat.shape[1]
    half = targets // CHAINS
    n_sg = rows // TILE
    n_tg = n_feat // n_sg
    th = half // n_tg
    n_fb, n_sb = feats // BIG, rows // BIG

    def hops(*by):
        return sum(min(d, side - d) for d in by)

    steps = range(side)
    plane = sorted([(a, b) for a in steps for b in steps if a or b], key=lambda o: hops(*o))
    far_first = sorted([(a, b, d) for a in steps for b in steps for d in steps if a or b or d],
                       key=lambda o: (-hops(*o), (o[0] + 3 * o[1] + 5 * o[2]) % 7))
    arrive = sorted(steps, key=lambda q: max(hops(*o) for o in far_first if sum(o) % side == q))
    per_sb = n_feat // n_sb
    total_rows = rows * n_samp

    me = lax.axis_index("feat")
    core = lax.axis_index("samp")

    barrier = pltpu.get_barrier_semaphore()

    def greet(d, _):
        pl.semaphore_signal(barrier, inc=1, device_id={"feat": (me + d) % n_feat}, device_id_type=MESH)
        return 0

    lax.fori_loop(1, n_feat, greet, 0)
    pl.semaphore_signal(barrier, inc=1, device_id={"samp": 1 - core}, device_id_type=MESH)

    w_load = pltpu.make_async_copy(w0_hbm, w_nat, in_sem.at[0])
    w_load.start()

    mz, my, mx = me // (side * side), (me // side) % side, me % side
    at_z, at_y = [lax.rem(mz + d, side) for d in steps], [lax.rem(my + d, side) for d in steps]
    my_sb, my_in_sb = (mx + my + mz) % side, mz * side + my
    pos = my_sb * per_sb + my_in_sb

    def class_of(k):
        return sum(jnp.where(k == i, q, 0) for i, q in enumerate(reversed(arrive)))

    def block_of(k):
        return lax.rem(my_sb + class_of(k), n_sb)

    def block_rows(k):
        return pl.ds(pl.multiple_of(block_of(k) * BIG, BIG), BIG)

    def x_load(k):
        return pltpu.make_async_copy(x_hbm.at[block_rows(k)], x_v.at[block_rows(k)], x_sem.at[k])

    x_load(0).start()
    my_sg, my_tg = pos // n_tg, pos % n_tg
    y_load = pltpu.make_async_copy(y_hbm.at[pl.ds(pl.multiple_of(my_sg * TILE, TILE), TILE)], y_tile, in_sem.at[1])

    def rs_copy(c, place, peer):
        return pltpu.make_async_remote_copy(src_ref=u_buf.at[c, place], dst_ref=rs_recv.at[c, pos], send_sem=rs_ssem.at[c],
                                            recv_sem=rs_rsem.at[c], device_id={"feat": peer}, device_id_type=MESH)

    def rs_all(c):
        return pltpu.make_async_remote_copy(src_ref=u_buf.at[c, pl.ds(1, n_feat - 1)], dst_ref=rs_recv.at[c, pl.ds(1, n_feat - 1)],
                                            send_sem=rs_ssem.at[c], recv_sem=rs_rsem.at[c], device_id={"feat": me},
                                            device_id_type=MESH)

    def keep_tiles(c, k, u):
        sb = block_of(k)
        for j in range(per_sb):
            g, t = j // n_tg, j % n_tg
            u_buf[c, sb * per_sb + j] = u[t * th:(t + 1) * th, g * TILE:(g + 1) * TILE].astype(jnp.bfloat16)

    def send_tiles(c, k):
        sb = block_of(k)

        def send(dz, dy, when):
            z, y = at_z[dz], at_y[dy]
            x = lax.rem(sb + 2 * side - z - y, side)
            column = z * side + y
            copy = rs_copy(c, sb * per_sb + column, column * side + x)
            if when is True:
                copy.start()
            else:
                pl.when(when)(copy.start)

        for a, b in reversed(plane):
            send(a, b, True)
        send(0, 0, k != n_sb - 1)

    def reduce(c, coef):
        rs_all(c).wait_recv()
        rs_recv[c, pos] = u_buf[c, pos]
        accs = [rs_recv[c, j].astype(jnp.float32) for j in range(4)]
        for j in range(4, n_feat):
            accs[j % 4] = accs[j % 4] + rs_recv[c, j].astype(jnp.float32)
        total = (accs[0] + accs[1]) + (accs[2] + accs[3])
        rs_res[c] = rs_res[c] - coef * total

    def place_of(device):
        z, y, x = device // (side * side), (device // side) % side, device % side
        return (x + y + z) % side * per_sb + z * side + y

    def axes(first_axis):
        kinds = (first_axis, (first_axis + 1) % 3, (first_axis + 2) % 3)
        strides = [jnp.where(d == 0, 1, jnp.where(d == 1, side, side * side)) for d in kinds]
        return [(stride, (me // stride) % side) for stride in strides]

    def moved(axis, by):
        stride, at = axis
        return ((at + by) % side - at) * stride

    def gather_copy(c, ref, place, peer, recv_sem):
        return pltpu.make_async_remote_copy(src_ref=ref.at[c, place], dst_ref=ref.at[c, place], send_sem=ag_ssem.at[c],
                                            recv_sem=recv_sem, device_id={"feat": peer}, device_id_type=MESH)

    def gather_start(c):
        moves = [[moved(axis, by) for by in range(side)] for axis in axes(core % 3)]
        for a, b, d in far_first:
            gather_copy(c, rb_full, pos, me + moves[0][a] + moves[1][b] + moves[2][d],
                        ag_rsem.at[c, (a + b + d) % side]).start()

    def pass_on(c, place):
        ring = axes((c * n_samp + core) % 3)[0]
        for d in range(side - 1, 0, -1):
            gather_copy(c, rf_full, place, me + moved(ring, d), ag_rsem.at[c, 0]).start()

    def last_gather_start(c):
        _, one, two = axes((c * n_samp + core) % 3)
        for i in range(len(plane) - 1, -1, -1):
            a, b = plane[i]
            gather_copy(c, rf_full, pos, me + moved(one, a) + moved(two, b), ag_psem.at[c, i]).start()
        pass_on(c, pos)

    def last_gather_forward(c):
        _, one, two = axes((c * n_samp + core) % 3)
        for i, (a, b) in enumerate(plane):
            place = place_of(me + moved(one, side - a) + moved(two, side - b))
            gather_copy(c, rf_full, place, me, ag_psem.at[c, i]).wait_recv()
            pass_on(c, place)

    def gather_wait(c, ref, tiles, q):
        part = ref.at[c, pl.ds(0, tiles)]
        pltpu.make_async_remote_copy(src_ref=part, dst_ref=part, send_sem=ag_ssem.at[c], recv_sem=ag_rsem.at[c, q],
                                     device_id={"feat": me}, device_id_type=MESH).wait_recv()

    def gather_sent(c, ref):
        part = ref.at[c, pl.ds(1, n_feat - 1)]
        pltpu.make_async_remote_copy(src_ref=part, dst_ref=part, send_sem=ag_ssem.at[c], recv_sem=ag_rsem.at[c, 0],
                                     device_id={"feat": me}, device_id_type=MESH).wait_send()

    def g_copy(c, par, f):
        return pltpu.make_async_remote_copy(src_ref=gt.at[c, f], dst_ref=g_recv.at[par, c, f], send_sem=g_ssem.at[c, f],
                                            recv_sem=g_rsem.at[par, c, f], device_id={"samp": 1 - core}, device_id_type=MESH)

    w_load.wait()
    for k in range(1, n_sb):
        x_load(k).start()
    y_load.start()
    for f in range(n_fb):
        wt = w_nat[f * BIG:(f + 1) * BIG, :].T
        for c in range(CHAINS):
            w_t[c, f] = wt[c * half:(c + 1) * half]
            st[c, :, f * BIG:(f + 1) * BIG] = wt[c * half:(c + 1) * half].astype(jnp.bfloat16)
    lam_t[...] = jnp.broadcast_to(lam_ref[...], (targets, targets)).T

    def first(k, _):
        x_load(k).wait()
        u = lax.dot_general(st[...].reshape(targets, feats), x_v[block_rows(k), :], (((1,), (1,)), ((), ())),
                            preferred_element_type=jnp.float32)
        for c in range(CHAINS):
            keep_tiles(c, k, u[c * half:(c + 1) * half])

        @pl.when(k == 0)
        def _():
            pl.semaphore_wait(barrier, n_feat)
        send_tiles(0, k)
        return 0

    lax.fori_loop(0, n_sb, first, 0)
    lax.fori_loop(0, n_sb, lambda k, _: (send_tiles(1, k), 0)[1], 0)

    eye = (lax.broadcasted_iota(jnp.int32, (MXU, MXU), 0) == lax.broadcasted_iota(jnp.int32, (MXU, MXU), 1)).astype(jnp.bfloat16)

    def turn(r, _):
        piece = pl.ds(pl.multiple_of(r * MXU, MXU), MXU)
        for f in range(0, feats, MXU):
            turned = lax.dot_general(eye, x_v[piece, f:f + MXU], (((1,), (1,)), ((), ())), preferred_element_type=jnp.float32)
            xt_v[f:f + MXU, piece] = turned.astype(jnp.bfloat16)
        return 0

    lax.fori_loop(0, rows // MXU // 2, turn, 0)
    y_load.wait()
    y_tile[...] = y_tile[...].T

    def behind(c, coef, last):
        reduce(c, coef)
        if last:
            rf_full[c, pos] = rs_res[c]
            last_gather_start(c)
        else:
            rb_full[c, pos] = rs_res[c].astype(jnp.bfloat16)
            gather_start(c)
        rs_all(c).wait_send()

    def gradient_part(c, par):
        for n, q in enumerate(arrive):
            gather_wait(c, rb_full, per_sb - (q == 0), q)
            sb = (my_sb + side - q) % n_sb
            block = pl.ds(pl.multiple_of(sb * BIG, BIG), BIG)
            rbt = jnp.concatenate([rb_full[c, pl.ds(sb * per_sb + g * n_tg, n_tg)].reshape(half, TILE) for g in range(BIG // TILE)], axis=1)
            for f in range(n_fb):
                part = jnp.dot(rbt, x_v[block, f * BIG:(f + 1) * BIG], preferred_element_type=jnp.float32)
                gt[c, f] = part if n == 0 else gt[c, f] + part
                if n == len(arrive) - 1:
                    g_copy(c, par, f).start()

    def step_and_product(c, par):
        lam = lam_t[c * half:(c + 1) * half, :]
        lam = jnp.concatenate([lam] * (BIG // targets), axis=1)

        def step(f, _):
            g_copy(c, par, f).wait_recv()
            cols = pl.ds(pl.multiple_of(f * BIG, BIG), BIG)
            gradient = (gt[c, f] + g_recv[par, c, f]) / total_rows
            w = w_t[c, f]
            delta = eta_ref[:, cols] * (gradient - lam * w)
            w_t[c, f] = w + STEP_WEIGHT * delta
            st[c, :, cols] = delta.astype(jnp.bfloat16)
            return 0

        lax.fori_loop(0, n_fb, step, 0)
        gather_sent(c, rb_full)

        def product(k, _):
            keep_tiles(c, k, jnp.dot(st[c], xt_v[:, block_rows(k)], preferred_element_type=jnp.float32))
            send_tiles(c, k)
            return 0

        lax.fori_loop(0, n_sb, product, 0)
        for f in range(n_fb):
            g_copy(c, par, f).wait_send()

    def sweep(s, last):
        par = s % 2
        for c in range(CHAINS):
            gradient_part(c, par)
        for c in range(CHAINS):
            step_and_product(c, par)
        if last:
            for f in range(n_fb):
                w_out[f * BIG:(f + 1) * BIG, :] = jnp.concatenate([w_t[c, f] for c in range(CHAINS)], axis=0).T
        for c in range(CHAINS):
            behind(c, STEP_WEIGHT, last)

    for c in range(CHAINS):
        rs_res[c] = y_tile[pl.ds(pl.multiple_of(c * half + my_tg * th, th), th), :]
    for c in range(CHAINS):
        behind(c, 1.0, False)
    lax.fori_loop(rows // MXU // 2, rows // MXU, turn, 0)
    lax.fori_loop(0, SWEEPS - 1, lambda s, _: (sweep(s, False), 0)[1], 0)
    sweep(SWEEPS - 1, True)
    for c in range(CHAINS):
        last_gather_forward(c)

    for c in range(CHAINS):
        gather_wait(c, rf_full, n_feat - side * side, 0)
    for g in range(n_sg):
        both = jnp.concatenate([rf_full[c, g * n_tg:(g + 1) * n_tg].reshape(half, TILE) for c in range(CHAINS)], axis=0)
        r_out[g * TILE:(g + 1) * TILE, :] = both.T
    for c in range(CHAINS):
        gather_sent(c, rf_full)


def _write(w_ref, r_ref, w_out, r_out, sem):
    copies = [pltpu.make_async_copy(w_ref, w_out, sem.at[0]), pltpu.make_async_copy(r_ref, r_out, sem.at[1])]
    for copy in copies:
        copy.start()
    for copy in copies:
        copy.wait()


def solution(mesh):
    n_samp, n_feat = mesh.shape["samp"], mesh.shape["feat"]
    side = round(n_feat ** (1 / 3))
    design_spec = P(("problem", "samp"), "feat")
    rows_spec = P(("problem", "samp"), None)
    coef_spec = P(("problem", "feat"), None)
    step_spec = P(("problem", "feat"))
    ridge_spec = P("problem")

    def local_sweeps(design, targets, coef_init, step_sizes, ridge_weights):
        rows, feats = design.shape
        tgt = targets.shape[1]
        half = tgt // CHAINS
        n_fb, n_sb = feats // BIG, rows // BIG
        n_tg = n_feat // (rows // TILE)
        th = half // n_tg
        f32, bf16 = jnp.float32, jnp.bfloat16
        hbm = pl.BlockSpec(memory_space=pl.ANY)
        vmem = pl.BlockSpec(memory_space=pltpu.VMEM)
        w, r = pl.pallas_call(
            functools.partial(_kernel, side, n_feat, n_samp),
            name="descent",
            out_shape=(pltpu.VMEM((feats, tgt), f32), pltpu.VMEM((rows, tgt), f32)),
            in_specs=[hbm, hbm, hbm, vmem, vmem],
            out_specs=(vmem, vmem),
            scratch_shapes=[
                pltpu.VMEM((rows, feats), bf16),
                pltpu.VMEM((feats, rows), bf16),
                pltpu.VMEM((feats, tgt), f32),
                pltpu.VMEM((CHAINS, n_fb, half, BIG), f32),
                pltpu.VMEM((CHAINS, half, feats), bf16),
                pltpu.VMEM((CHAINS, n_feat, th, TILE), bf16),
                pltpu.VMEM((CHAINS, n_feat, th, TILE), bf16),
                pltpu.VMEM((CHAINS, n_feat, th, TILE), bf16),
                pltpu.VMEM((CHAINS, n_fb, half, BIG), f32),
                pltpu.VMEM((2, CHAINS, n_fb, half, BIG), f32),
                pltpu.VMEM((CHAINS, th, TILE), f32),
                pltpu.VMEM((CHAINS, n_feat, th, TILE), f32),
                pltpu.VMEM((TILE, tgt), f32),
                pltpu.VMEM((tgt, tgt), f32),
                pltpu.SemaphoreType.DMA((n_sb,)),
                pltpu.SemaphoreType.DMA((2,)),
                pltpu.SemaphoreType.DMA((CHAINS,)),
                pltpu.SemaphoreType.DMA((CHAINS,)),
                pltpu.SemaphoreType.DMA((CHAINS,)),
                pltpu.SemaphoreType.DMA((CHAINS, side * side)),
                pltpu.SemaphoreType.DMA((CHAINS, side)),
                pltpu.SemaphoreType.DMA((CHAINS, n_fb)),
                pltpu.SemaphoreType.DMA((2, CHAINS, n_fb)),
            ],
            compiler_params=pltpu.CompilerParams(collective_id=0, has_side_effects=True, vmem_limit_bytes=56 * 1024 * 1024),
        )(design, targets, coef_init, step_sizes[None, :], ridge_weights[None, :])
        return pl.pallas_call(
            _write,
            name="write",
            out_shape=(jax.ShapeDtypeStruct(w.shape, f32), jax.ShapeDtypeStruct(r.shape, f32)),
            in_specs=[vmem, vmem],
            out_specs=(hbm, hbm),
            scratch_shapes=[pltpu.SemaphoreType.DMA((2,))],
        )(pltpu.with_memory_space_constraint(w, pltpu.VMEM), pltpu.with_memory_space_constraint(r, pltpu.VMEM))

    return jax.shard_map(local_sweeps, mesh=mesh, in_specs=(design_spec, rows_spec, coef_spec, step_spec, ridge_spec), out_specs=(coef_spec, rows_spec), check_vma=False)
```

```python
import functools

import jax
import jax.numpy as jnp
from jax import lax
from jax.experimental import pallas as pl
from jax.experimental.pallas import tpu as pltpu
from jax.sharding import PartitionSpec as P

SWEEPS = 4
STEP_WEIGHT = 0.5
CHAINS = 2
TILE = 128
BIG = 512
MXU = 256
MESH = pl.DeviceIdType.MESH


def _kernel(side, n_feat, n_samp, x_hbm, y_hbm, w0_hbm, eta_ref, lam_ref, w_out, r_out,
            x_v, xt_v, w_nat, w_t, st, u_buf, rs_recv, rb_full, gt, g_recv, rs_res, rf_full, y_tile, lam_t,
            x_sem, in_sem, rs_ssem, rs_rsem, ag_ssem, ag_psem, ag_rsem, g_ssem, g_rsem):
    rows, feats = x_v.shape
    targets = w_nat.shape[1]
    half = targets // CHAINS
    n_sg = rows // TILE
    n_tg = n_feat // n_sg
    th = half // n_tg
    n_fb, n_sb = feats // BIG, rows // BIG

    def hops(*by):
        return sum(min(d, side - d) for d in by)

    steps = range(side)
    plane = sorted([(a, b) for a in steps for b in steps if a or b], key=lambda o: hops(*o))
    far_first = sorted([(a, b, d) for a in steps for b in steps for d in steps if a or b or d],
                       key=lambda o: (-hops(*o), (o[0] + 3 * o[1] + 5 * o[2]) % 7))
    arrive = sorted(steps, key=lambda q: max(hops(*o) for o in far_first if sum(o) % side == q))
    per_sb = n_feat // n_sb
    total_rows = rows * n_samp

    me = lax.axis_index("feat")
    core = lax.axis_index("samp")

    barrier = pltpu.get_barrier_semaphore()

    def greet(d, _):
        pl.semaphore_signal(barrier, inc=1, device_id={"feat": (me + d) % n_feat}, device_id_type=MESH)
        return 0

    lax.fori_loop(1, n_feat, greet, 0)
    pl.semaphore_signal(barrier, inc=1, device_id={"samp": 1 - core}, device_id_type=MESH)

    w_load = pltpu.make_async_copy(w0_hbm, w_nat, in_sem.at[0])
    w_load.start()

    mz, my, mx = me // (side * side), (me // side) % side, me % side
    at_z, at_y = [lax.rem(mz + d, side) for d in steps], [lax.rem(my + d, side) for d in steps]
    my_sb, my_in_sb = (mx + my + mz) % side, mz * side + my
    pos = my_sb * per_sb + my_in_sb

    def class_of(k):
        return sum(jnp.where(k == i, q, 0) for i, q in enumerate(reversed(arrive)))

    def block_of(k):
        return lax.rem(my_sb + class_of(k), n_sb)

    def block_rows(k):
        return pl.ds(pl.multiple_of(block_of(k) * BIG, BIG), BIG)

    def x_load(k):
        return pltpu.make_async_copy(x_hbm.at[block_rows(k)], x_v.at[block_rows(k)], x_sem.at[k])

    x_load(0).start()
    my_sg, my_tg = pos // n_tg, pos % n_tg
    y_load = pltpu.make_async_copy(y_hbm.at[pl.ds(pl.multiple_of(my_sg * TILE, TILE), TILE)], y_tile, in_sem.at[1])

    def rs_copy(c, place, peer):
        return pltpu.make_async_remote_copy(src_ref=u_buf.at[c, place], dst_ref=rs_recv.at[c, pos], send_sem=rs_ssem.at[c],
                                            recv_sem=rs_rsem.at[c], device_id={"feat": peer}, device_id_type=MESH)

    def rs_all(c):
        return pltpu.make_async_remote_copy(src_ref=u_buf.at[c, pl.ds(1, n_feat - 1)], dst_ref=rs_recv.at[c, pl.ds(1, n_feat - 1)],
                                            send_sem=rs_ssem.at[c], recv_sem=rs_rsem.at[c], device_id={"feat": me},
                                            device_id_type=MESH)

    def keep_tiles(c, k, u):
        sb = block_of(k)
        for j in range(per_sb):
            g, t = j // n_tg, j % n_tg
            u_buf[c, sb * per_sb + j] = u[t * th:(t + 1) * th, g * TILE:(g + 1) * TILE].astype(jnp.bfloat16)

    def send_tiles(c, k):
        sb = block_of(k)

        def send(dz, dy, when):
            z, y = at_z[dz], at_y[dy]
            x = lax.rem(sb + 2 * side - z - y, side)
            column = z * side + y
            copy = rs_copy(c, sb * per_sb + column, column * side + x)
            if when is True:
                copy.start()
            else:
                pl.when(when)(copy.start)

        for a, b in reversed(plane):
            send(a, b, True)
        send(0, 0, k != n_sb - 1)

    def reduce(c, coef):
        rs_all(c).wait_recv()
        rs_recv[c, pos] = u_buf[c, pos]
        accs = [rs_recv[c, j].astype(jnp.float32) for j in range(4)]
        for j in range(4, n_feat):
            accs[j % 4] = accs[j % 4] + rs_recv[c, j].astype(jnp.float32)
        total = (accs[0] + accs[1]) + (accs[2] + accs[3])
        rs_res[c] = rs_res[c] - coef * total

    def place_of(device):
        z, y, x = device // (side * side), (device // side) % side, device % side
        return (x + y + z) % side * per_sb + z * side + y

    def axes(first_axis):
        kinds = (first_axis, (first_axis + 1) % 3, (first_axis + 2) % 3)
        strides = [jnp.where(d == 0, 1, jnp.where(d == 1, side, side * side)) for d in kinds]
        return [(stride, (me // stride) % side) for stride in strides]

    def moved(axis, by):
        stride, at = axis
        return ((at + by) % side - at) * stride

    def gather_copy(c, ref, place, peer, recv_sem):
        return pltpu.make_async_remote_copy(src_ref=ref.at[c, place], dst_ref=ref.at[c, place], send_sem=ag_ssem.at[c],
                                            recv_sem=recv_sem, device_id={"feat": peer}, device_id_type=MESH)

    def gather_start(c):
        moves = [[moved(axis, by) for by in range(side)] for axis in axes(core % 3)]
        for a, b, d in far_first:
            gather_copy(c, rb_full, pos, me + moves[0][a] + moves[1][b] + moves[2][d],
                        ag_rsem.at[c, (a + b + d) % side]).start()

    def pass_on(c, place):
        ring = axes((c * n_samp + core) % 3)[0]
        for d in range(side - 1, 0, -1):
            gather_copy(c, rf_full, place, me + moved(ring, d), ag_rsem.at[c, 0]).start()

    def last_gather_start(c):
        _, one, two = axes((c * n_samp + core) % 3)
        for i in range(len(plane) - 1, -1, -1):
            a, b = plane[i]
            gather_copy(c, rf_full, pos, me + moved(one, a) + moved(two, b), ag_psem.at[c, i]).start()
        pass_on(c, pos)

    def last_gather_forward(c):
        _, one, two = axes((c * n_samp + core) % 3)
        for i, (a, b) in enumerate(plane):
            place = place_of(me + moved(one, side - a) + moved(two, side - b))
            gather_copy(c, rf_full, place, me, ag_psem.at[c, i]).wait_recv()
            pass_on(c, place)

    def gather_wait(c, ref, tiles, q):
        part = ref.at[c, pl.ds(0, tiles)]
        pltpu.make_async_remote_copy(src_ref=part, dst_ref=part, send_sem=ag_ssem.at[c], recv_sem=ag_rsem.at[c, q],
                                     device_id={"feat": me}, device_id_type=MESH).wait_recv()

    def gather_sent(c, ref):
        part = ref.at[c, pl.ds(1, n_feat - 1)]
        pltpu.make_async_remote_copy(src_ref=part, dst_ref=part, send_sem=ag_ssem.at[c], recv_sem=ag_rsem.at[c, 0],
                                     device_id={"feat": me}, device_id_type=MESH).wait_send()

    def g_copy(c, par, f):
        return pltpu.make_async_remote_copy(src_ref=gt.at[c, f], dst_ref=g_recv.at[par, c, f], send_sem=g_ssem.at[c, f],
                                            recv_sem=g_rsem.at[par, c, f], device_id={"samp": 1 - core}, device_id_type=MESH)

    w_load.wait()
    for k in range(1, n_sb):
        x_load(k).start()
    y_load.start()
    for f in range(n_fb):
        wt = w_nat[f * BIG:(f + 1) * BIG, :].T
        for c in range(CHAINS):
            w_t[c, f] = wt[c * half:(c + 1) * half]
            st[c, :, f * BIG:(f + 1) * BIG] = wt[c * half:(c + 1) * half].astype(jnp.bfloat16)
    lam_t[...] = jnp.broadcast_to(lam_ref[...], (targets, targets)).T

    def first(k, _):
        x_load(k).wait()
        u = lax.dot_general(st[...].reshape(targets, feats), x_v[block_rows(k), :], (((1,), (1,)), ((), ())),
                            preferred_element_type=jnp.float32)
        for c in range(CHAINS):
            keep_tiles(c, k, u[c * half:(c + 1) * half])

        @pl.when(k == 0)
        def _():
            pl.semaphore_wait(barrier, n_feat)
        send_tiles(0, k)
        return 0

    lax.fori_loop(0, n_sb, first, 0)
    lax.fori_loop(0, n_sb, lambda k, _: (send_tiles(1, k), 0)[1], 0)

    eye = (lax.broadcasted_iota(jnp.int32, (MXU, MXU), 0) == lax.broadcasted_iota(jnp.int32, (MXU, MXU), 1)).astype(jnp.bfloat16)

    def turn(r, _):
        piece = pl.ds(pl.multiple_of(r * MXU, MXU), MXU)
        for f in range(0, feats, MXU):
            turned = lax.dot_general(eye, x_v[piece, f:f + MXU], (((1,), (1,)), ((), ())), preferred_element_type=jnp.float32)
            xt_v[f:f + MXU, piece] = turned.astype(jnp.bfloat16)
        return 0

    lax.fori_loop(0, rows // MXU // 2, turn, 0)
    y_load.wait()
    y_tile[...] = y_tile[...].T

    def behind(c, coef, last):
        reduce(c, coef)
        if last:
            rf_full[c, pos] = rs_res[c]
            last_gather_start(c)
        else:
            rb_full[c, pos] = rs_res[c].astype(jnp.bfloat16)
            gather_start(c)
        rs_all(c).wait_send()

    def gradient_part(c, par):
        for n, q in enumerate(arrive):
            gather_wait(c, rb_full, per_sb - (q == 0), q)
            sb = (my_sb + side - q) % n_sb
            block = pl.ds(pl.multiple_of(sb * BIG, BIG), BIG)
            rbt = jnp.concatenate([rb_full[c, pl.ds(sb * per_sb + g * n_tg, n_tg)].reshape(half, TILE) for g in range(BIG // TILE)], axis=1)
            for f in range(n_fb):
                part = jnp.dot(rbt, x_v[block, f * BIG:(f + 1) * BIG], preferred_element_type=jnp.float32)
                gt[c, f] = part if n == 0 else gt[c, f] + part
                if n == len(arrive) - 1:
                    g_copy(c, par, f).start()

    def step_and_product(c, par):
        lam = lam_t[c * half:(c + 1) * half, :]
        lam = jnp.concatenate([lam] * (BIG // targets), axis=1)

        def step(f, _):
            g_copy(c, par, f).wait_recv()
            cols = pl.ds(pl.multiple_of(f * BIG, BIG), BIG)
            gradient = (gt[c, f] + g_recv[par, c, f]) / total_rows
            w = w_t[c, f]
            delta = eta_ref[:, cols] * (gradient - lam * w)
            w_t[c, f] = w + STEP_WEIGHT * delta
            st[c, :, cols] = delta.astype(jnp.bfloat16)
            return 0

        lax.fori_loop(0, n_fb, step, 0)
        gather_sent(c, rb_full)

        def product(k, _):
            keep_tiles(c, k, jnp.dot(st[c], xt_v[:, block_rows(k)], preferred_element_type=jnp.float32))
            send_tiles(c, k)
            return 0

        lax.fori_loop(0, n_sb, product, 0)
        for f in range(n_fb):
            g_copy(c, par, f).wait_send()

    def sweep(s, last):
        par = s % 2
        for c in range(CHAINS):
            gradient_part(c, par)
        for c in range(CHAINS):
            step_and_product(c, par)
        if last:
            for f in range(n_fb):
                w_out[f * BIG:(f + 1) * BIG, :] = jnp.concatenate([w_t[c, f] for c in range(CHAINS)], axis=0).T
        for c in range(CHAINS):
            behind(c, STEP_WEIGHT, last)

    for c in range(CHAINS):
        rs_res[c] = y_tile[pl.ds(pl.multiple_of(c * half + my_tg * th, th), th), :]
    for c in range(CHAINS):
        behind(c, 1.0, False)
    lax.fori_loop(rows // MXU // 2, rows // MXU, turn, 0)
    lax.fori_loop(0, SWEEPS - 1, lambda s, _: (sweep(s, False), 0)[1], 0)
    sweep(SWEEPS - 1, True)
    for c in range(CHAINS):
        last_gather_forward(c)

    for c in range(CHAINS):
        gather_wait(c, rf_full, n_feat - side * side, 0)
        for g in range(n_sg):
            r_out[g * TILE:(g + 1) * TILE, c * half:(c + 1) * half] = rf_full[c, g * n_tg:(g + 1) * n_tg].reshape(half, TILE).T
    for c in range(CHAINS):
        gather_sent(c, rf_full)


def _write(w_ref, r_ref, w_out, r_out, sem):
    copies = [pltpu.make_async_copy(w_ref, w_out, sem.at[0]), pltpu.make_async_copy(r_ref, r_out, sem.at[1])]
    for copy in copies:
        copy.start()
    for copy in copies:
        copy.wait()


def solution(mesh):
    n_samp, n_feat = mesh.shape["samp"], mesh.shape["feat"]
    side = round(n_feat ** (1 / 3))
    design_spec = P(("problem", "samp"), "feat")
    rows_spec = P(("problem", "samp"), None)
    coef_spec = P(("problem", "feat"), None)
    step_spec = P(("problem", "feat"))
    ridge_spec = P("problem")

    def local_sweeps(design, targets, coef_init, step_sizes, ridge_weights):
        rows, feats = design.shape
        tgt = targets.shape[1]
        half = tgt // CHAINS
        n_fb, n_sb = feats // BIG, rows // BIG
        n_tg = n_feat // (rows // TILE)
        th = half // n_tg
        f32, bf16 = jnp.float32, jnp.bfloat16
        hbm = pl.BlockSpec(memory_space=pl.ANY)
        vmem = pl.BlockSpec(memory_space=pltpu.VMEM)
        w, r = pl.pallas_call(
            functools.partial(_kernel, side, n_feat, n_samp),
            name="descent",
            out_shape=(pltpu.VMEM((feats, tgt), f32), pltpu.VMEM((rows, tgt), f32)),
            in_specs=[hbm, hbm, hbm, vmem, vmem],
            out_specs=(vmem, vmem),
            scratch_shapes=[
                pltpu.VMEM((rows, feats), bf16),
                pltpu.VMEM((feats, rows), bf16),
                pltpu.VMEM((feats, tgt), f32),
                pltpu.VMEM((CHAINS, n_fb, half, BIG), f32),
                pltpu.VMEM((CHAINS, half, feats), bf16),
                pltpu.VMEM((CHAINS, n_feat, th, TILE), bf16),
                pltpu.VMEM((CHAINS, n_feat, th, TILE), bf16),
                pltpu.VMEM((CHAINS, n_feat, th, TILE), bf16),
                pltpu.VMEM((CHAINS, n_fb, half, BIG), f32),
                pltpu.VMEM((2, CHAINS, n_fb, half, BIG), f32),
                pltpu.VMEM((CHAINS, th, TILE), f32),
                pltpu.VMEM((CHAINS, n_feat, th, TILE), f32),
                pltpu.VMEM((TILE, tgt), f32),
                pltpu.VMEM((tgt, tgt), f32),
                pltpu.SemaphoreType.DMA((n_sb,)),
                pltpu.SemaphoreType.DMA((2,)),
                pltpu.SemaphoreType.DMA((CHAINS,)),
                pltpu.SemaphoreType.DMA((CHAINS,)),
                pltpu.SemaphoreType.DMA((CHAINS,)),
                pltpu.SemaphoreType.DMA((CHAINS, side * side)),
                pltpu.SemaphoreType.DMA((CHAINS, side)),
                pltpu.SemaphoreType.DMA((CHAINS, n_fb)),
                pltpu.SemaphoreType.DMA((2, CHAINS, n_fb)),
            ],
            compiler_params=pltpu.CompilerParams(collective_id=0, has_side_effects=True, vmem_limit_bytes=56 * 1024 * 1024),
        )(design, targets, coef_init, step_sizes[None, :], ridge_weights[None, :])
        return pl.pallas_call(
            _write,
            name="write",
            out_shape=(jax.ShapeDtypeStruct(w.shape, f32), jax.ShapeDtypeStruct(r.shape, f32)),
            in_specs=[vmem, vmem],
            out_specs=(hbm, hbm),
            scratch_shapes=[pltpu.SemaphoreType.DMA((2,))],
        )(pltpu.with_memory_space_constraint(w, pltpu.VMEM), pltpu.with_memory_space_constraint(r, pltpu.VMEM))

    return jax.shard_map(local_sweeps, mesh=mesh, in_specs=(design_spec, rows_spec, coef_spec, step_spec, ridge_spec), out_specs=(coef_spec, rows_spec), check_vma=False)
```
